256 devices in a mesh: lon: 16 (over x_hi, y, core), dp: 16 (over z, x_lo).
Axes of the slice: x: 4 (x_hi: 2, x_lo: 2; x = x_hi * 2 + x_lo), y: 4, z: 8, core: 2. Of those that a mesh axis runs over, the one named last changes fastest.
Arguments:
- inputs: bfloat16 [16, 32, 768, 256], P('dp', None, 'lon'), may hold values from -6 to 6
- pre_act: bfloat16 [16, 32, 768, 256], P('dp', None, 'lon'), may hold values from -6 to 6
- cotangent: bfloat16 [16, 32, 768, 256], P('dp', None, 'lon'), may hold values from -6 to 6
- first_weight: bfloat16 [2304, 256], replicated, may hold values from -0.125 to 0.125
- second_weight: bfloat16 [2304, 256], replicated, may hold values from -0.125 to 0.125
Outputs:
- input_gradient_array: bfloat16 [16, 32, 768, 256], P('dp', None, 'lon')
- first_weight_gradient: float32 [589824], P(('lon', 'dp'))
- second_weight_gradient: float32 [589824], P(('lon', 'dp'))
The draws below stay inside these ranges and needn't reach their ends.
All inputs are finite; a program needn't handle non-finite values.
Results may differ from the reference program's by a relative error of at most 0.0049.
Values may be sent and summed in bfloat16 or wider, within the bound.
A program may use at most 64 MiB of HBM per device.

```python
import jax
import jax.numpy as jnp

C = 256
FIRST_SPREAD = 12
SECOND_SPREAD = 18
LAT = 32
NLON = 768
SAMPLES = 16


def shard_levels(stream_key, shape, split, least, largest):
    def one(axis_at, blocks):
        steps = jax.random.uniform(jax.random.fold_in(jax.random.fold_in(stream_key, 6), axis_at), (blocks,), jnp.float32, least / len(split), largest / len(split))
        return jnp.repeat(jnp.exp(steps), shape[axis_at] // blocks).reshape((-1,) + (1,) * (len(shape) - axis_at - 1))

    level = one(*split[0])
    for cut in split[1:]:
        level = level * one(*cut)
    return level


def bell_draw(key, extent, scale, bound, cuts=(), held_as=jnp.bfloat16):
    result = scale * jax.random.normal(key, extent, jnp.float32)
    if cuts:
        result = result * shard_levels(key, extent, cuts, -0.22, 0.18)
    return jnp.clip(result, -bound, bound).astype(held_as)


def setup_inputs(seed: int = 0) -> dict:
    seeds = jax.random.split(jax.random.key(seed), 6)
    return {
        "inputs": bell_draw(seeds[0], (SAMPLES, LAT, NLON, C), 1.0, 6.0, ((0, 16), (2, 16))),
        "pre_act": bell_draw(seeds[1], (SAMPLES, LAT, NLON, C), 1.0, 6.0, ((0, 16), (2, 16))),
        "cotangent": bell_draw(seeds[2], (SAMPLES, LAT, NLON, C), 1.0, 6.0, ((0, 16), (2, 16))),
        "first_weight": bell_draw(seeds[3], (9 * C, C), (9 * C) ** -0.5, 0.125),
        "second_weight": bell_draw(seeds[4], (9 * C, C), (9 * C) ** -0.5, 0.125),
    }


def lat_move(values, offset):
    rows = values.shape[1]
    if abs(offset) >= rows:
        return jnp.zeros_like(values)
    if offset == 0:
        return values
    blank = jnp.zeros_like(values[:, :abs(offset)])
    if offset > 0:
        return jnp.concatenate([values[:, offset:], blank], axis=1)
    return jnp.concatenate([blank, values[:, :rows + offset]], axis=1)


def shifted(values, dilation, tap, direction):
    lat_off = direction * (tap // 3 - 1) * dilation
    lon_off = direction * (tap % 3 - 1) * dilation
    return lat_move(jnp.roll(values, -lon_off, axis=2), lat_off)


def kernel_weight_gradient(source, dilation, upstream):
    chans = upstream.shape[3]
    flat_up = upstream.reshape(-1, chans)
    blocks = []
    for tap in range(9):
        moved = shifted(source, dilation, tap, 1).reshape(-1, source.shape[3])
        blocks.append(jnp.dot(moved.T, flat_up, preferred_element_type=jnp.float32))
    return jnp.concatenate(blocks, axis=0)


def gradient_wrt_input(upstream, dilation, weights):
    chans = weights.shape[1]
    total = jnp.zeros((upstream.shape[0] * upstream.shape[1] * upstream.shape[2], weights.shape[1]), jnp.float32)
    for tap in range(9):
        moved = shifted(upstream, dilation, tap, -1).reshape(-1, chans)
        block = weights[tap * chans:(tap + 1) * chans]
        total = total + jnp.dot(moved, block.T, preferred_element_type=jnp.float32)
    return total.reshape(upstream.shape)


def reference(inputs, pre_act, cotangent, first_weight, second_weight):
    norm_factor = float(SAMPLES * LAT * NLON) ** -0.5
    hidden_activation = jnp.maximum(pre_act, jnp.zeros_like(pre_act))
    second_weight_gradient = (kernel_weight_gradient(hidden_activation, SECOND_SPREAD, cotangent) * norm_factor).reshape(-1)
    hidden_gradient = gradient_wrt_input(cotangent, SECOND_SPREAD, second_weight)
    partial_gradient = jnp.where(pre_act > 0, hidden_gradient, jnp.float32(0.0)).astype(jnp.bfloat16)
    first_weight_gradient = (kernel_weight_gradient(inputs, FIRST_SPREAD, partial_gradient) * norm_factor).reshape(-1)
    input_gradient_array = gradient_wrt_input(partial_gradient, FIRST_SPREAD, first_weight).astype(jnp.bfloat16)
    return input_gradient_array, first_weight_gradient, second_weight_gradient
```

```python
import jax
import jax.numpy as jnp
from jax import lax
from jax.experimental import pallas as pl
from jax.experimental.pallas import tpu as pltpu
from jax.sharding import PartitionSpec as P

BF = jnp.bfloat16
F32 = jnp.float32
LAT = 32
COLS = 48
CH = 256
HALF = 128
CELLS = LAT * COLS
LONS = 16
DPS = 16
ROWS = 9 * CH
BLOCK = ROWS // LONS
UNIT = BLOCK // DPS
PAD2 = 96
PAD1 = 64
W2 = 18
W1 = 12
M2 = 384
M1 = 256
MESH = pl.DeviceIdType.MESH
FAR_FIRST = sorted(range(1, DPS), key=lambda d: -min(d, DPS - d))
scope = jax.named_scope


def mm(a, b):
    return jnp.dot(a, b, preferred_element_type=F32)


def kernel(cot, pre2, x2, w1, w2, dx, g1, g2,
           V2, V1, S2, R2, S1, R1, pre, xin, w1b, w2b, wt1, wt2, hT, xT, acc, obuf,
           wf, wb, recvA, sY, sX, rY1, rX1, tY, tX, rY2, rX2, tYo, sC, sendD, recvD, gbuf,
           ld, st, hs, hr, as_, ar, ys, yr, xs, xr, ds_, dr, know1, know2):
    lon = lax.axis_index("lon")
    dp = lax.axis_index("dp")
    core = lax.rem(lon, 2)
    y = lax.rem(lax.div(lon, 2), 4)
    xh = lax.div(lon, 8)
    left = lax.rem(lon + LONS - 1, LONS)
    right = lax.rem(lon + 1, LONS)
    partner = lon + 1 - 2 * core
    ypeer = [lax.rem(y + d, 4) for d in range(1, 4)]
    ylon = [xh * 8 + yp * 2 + core for yp in ypeer]
    xlon = (1 - xh) * 8 + y * 2 + core
    dpeer = {d: lax.rem(dp + d, DPS) for d in range(1, DPS)}
    twin = dp + 1 - 2 * lax.rem(dp, 2)

    loads = []
    for i, (s, d) in enumerate((
        (cot, V2.at[1, PAD2:PAD2 + CELLS]), (w2, w2b), (pre2, pre), (x2, xin), (w1, w1b),
    )):
        c = pltpu.make_async_copy(s, d, ld.at[i])
        c.start()
        loads.append(c)

    barrier = pltpu.get_barrier_semaphore()

    def tell(sem, l, d):
        pl.semaphore_signal(sem, inc=1, device_id=(l, d), device_id_type=MESH)

    for l in [left, right, xlon] + ylon:
        tell(barrier, l, dp)
    for d in (dpeer[2], dpeer[14], dpeer[4], dpeer[12], twin):
        tell(barrier, lon, d)

    for c in range(3):
        V2[c, 0:PAD2] = jnp.zeros((PAD2, CH), BF)
        V2[c, PAD2 + CELLS:] = jnp.zeros((PAD2, CH), BF)
        V1[c, 0:PAD1] = jnp.zeros((PAD1, CH), BF)
        V1[c, PAD1 + CELLS:] = jnp.zeros((PAD1, CH), BF)
    for h in range(2):
        sC[h, BLOCK:] = jnp.zeros((16, HALF), F32)

    def remote(s, d, ss, rs, l, dd):
        c = pltpu.make_async_remote_copy(
            src_ref=s, dst_ref=d, send_sem=ss, recv_sem=rs,
            device_id=(l, dd), device_id_type=MESH)
        c.start()
        return c

    def wait_all(ref, sem):
        pltpu.make_async_copy(ref, ref, sem).wait()

    sent = []

    def pack(V, pad, S, w):
        for p in range(LAT):
            o = pad + p * COLS
            S[0, p * w:(p + 1) * w] = V[1, o + COLS - w:o + COLS]
            S[1, p * w:(p + 1) * w] = V[1, o:o + w]

    def build_inner(V, pad, w):
        for p in range(LAT):
            o = pad + p * COLS
            V[0, o:o + COLS - w] = V[1, o + w:o + COLS]
            V[2, o + w:o + COLS] = V[1, o:o + COLS - w]

    def build_edge(V, pad, R, w):
        for p in range(LAT):
            o = pad + p * COLS
            V[0, o + COLS - w:o + COLS] = R[1, p * w:(p + 1) * w]
            V[2, o:o + w] = R[0, p * w:(p + 1) * w]

    def send_halo(S, R, i):
        return [
            remote(S.at[0], R.at[0], hs.at[i], hr.at[i], right, dp),
            remote(S.at[1], R.at[1], hs.at[i + 1], hr.at[i + 1], left, dp),
        ]

    with scope("ld0"):
        loads[0].wait()
    with scope("pack2"):
        pack(V2, PAD2, S2, W2)
    with scope("barrier"):
        pl.semaphore_wait(barrier, 11)
    halo2 = send_halo(S2, R2, 0)
    for d in (dpeer[4], dpeer[12]):
        tell(know1, lon, d)
    with scope("inner2"):
        build_inner(V2, PAD2, W2)

    def tr_weights(w, wt):
        for c in range(3):
            for r in range(3):
                k = 3 * r + c
                wt[c, r * CH:(r + 1) * CH] = w[k * CH:(k + 1) * CH].T

    with scope("trans2"):
        loads[1].wait()
        tr_weights(w2b, wt2)
        loads[2].wait()
        for i in range(6):
            rows = pl.ds(i * CH, CH)
            hT[:, rows] = jnp.maximum(pre[rows], jnp.zeros((CH, CH), BF)).T

    blocks2 = ((0, 768, ((0, 960), (1, 96))), (768, 768, ((1, 864), (2, 0))))
    blocks1 = ((0, 512, ((0, 640), (1, 64))),
               (512, 512, ((0, 1152), (1, 576), (2, 0))),
               (1024, 512, ((1, 1088), (2, 512))))

    def dx_part(V, wt, cols, block, i, m):
        taps = block[2]
        lhs, rhs = [], []
        for c in cols:
            for r, s in taps:
                lhs.append(V[c, pl.ds(pl.multiple_of(s + i * m, 16), m)])
            rhs.append(wt[c, taps[0][0] * CH:(taps[-1][0] + 1) * CH])
        return mm(jnp.concatenate(lhs, axis=1), jnp.concatenate(rhs, axis=0))

    def dx_loop(V, wt, cols, blocks, m, put):
        for b in blocks:
            @pl.loop(0, b[1] // m)
            def _(i, b=b):
                put(pl.multiple_of(b[0] + i * m, m), dx_part(V, wt, cols, b, i, m))

    cells2 = ((0, 768, 960), (0, 1536, 96), (768, 768, 0))
    cells1 = ((0, 1024, 640), (0, 1536, 64), (512, 1024, 0))

    def dw(g, srcT, V, cells, cols):
        for c in cols:
            for r in range(3):
                a, n, s = cells[r]
                v = mm(srcT[:, a:a + n], V[c, s:s + n])
                k = 3 * r + c
                wf[g, k * CH:(k + 1) * CH] = v
                wb[g, k * CH:(k + 1) * CH] = v.astype(BF)

    def first2(m0, v):
        acc[pl.ds(m0, M2)] = v

    def mask2(m0, v):
        rows = pl.ds(m0, M2)
        lg = jnp.where(pre[rows].astype(F32) > 0, acc[rows] + v, 0.0).astype(BF)
        V1[1, pl.ds(pl.multiple_of(PAD1 + m0, 16), M2)] = lg

    def first1(m0, v):
        acc[pl.ds(m0, M1)] = v

    def last1(m0, v):
        rows = pl.ds(m0, M1)
        obuf[rows] = (acc[rows] + v).astype(BF)

    with scope("dx2c"):
        dx_loop(V2, wt2, (1,), blocks2, M2, first2)
    with scope("dw2c"):
        dw(1, hT, V2, cells2, (1,))
    with scope("know1"):
        pl.semaphore_wait(know1, 2)
        tell(know2, lon, twin)
    with scope("trans1"):
        loads[3].wait()
        for i in range(6):
            rows = pl.ds(i * CH, CH)
            xT[:, rows] = xin[rows].T
        loads[4].wait()
        tr_weights(w1b, wt1)

    with scope("halo2w"):
        for h in halo2:
            h.wait_recv()
    with scope("edge2"):
        build_edge(V2, PAD2, R2, W2)
    with scope("dx2lr"):
        dx_loop(V2, wt2, (0, 2), blocks2, M2, mask2)
    with scope("pack1"):
        pack(V1, PAD1, S1, W1)
    halo1 = send_halo(S1, R1, 2)
    with scope("dw2lr"):
        dw(1, hT, V2, cells2, (0, 2))

    def stage_a(g):
        for j in range(8):
            rows = pl.ds(pl.multiple_of((2 * j + 1 - core) * BLOCK, 16), BLOCK)
            remote(wb.at[g, rows], recvA.at[g, j], as_.at[g], ar.at[g], partner, dp)
        sent.append((recvA.at[g], as_.at[g]))

    def stage_b(g):
        wait_all(recvA.at[g], ar.at[g])

        @pl.loop(0, 8)
        def _(j):
            rows = pl.ds(pl.multiple_of((2 * j + core) * BLOCK, 16), BLOCK)
            v = (wf[g, rows] + recvA[g, j].astype(F32)).astype(BF)
            sY[g, lax.div(j, 4), lax.rem(j, 4)] = v[:, :HALF]
            sX[g, lax.div(j, 4), lax.rem(j, 4)] = v[:, HALF:]

        remote(sX.at[g, 1 - xh], rX1.at[g], xs.at[g, 0], xr.at[g, 0], xlon, dp)
        for d in (1, 0, 2):
            remote(sY.at[g, :, ypeer[d]], rY1.at[g, d], ys.at[g, 0], yr.at[g, 0], ylon[d], dp)
        sent.extend(((rX1.at[g], xs.at[g, 0]), (rY1.at[g], ys.at[g, 0])))

    def stage_cy(g):
        wait_all(rY1.at[g], yr.at[g, 0])
        for own, h in ((False, 1 - xh), (True, xh)):
            v = sY[g, h, y].astype(F32)
            for d in range(3):
                v = v + rY1[g, d, h].astype(F32)
            if own:
                tYo[g] = v
            else:
                tY[g] = v.astype(BF)
        remote(tY.at[g], rY2.at[g], xs.at[g, 1], xr.at[g, 1], xlon, dp)
        sent.append((rY2.at[g], xs.at[g, 1]))

    def stage_cx(g):
        wait_all(rX1.at[g], xr.at[g, 0])
        for i in range(4):
            tX[g, i] = (sX[g, xh, i].astype(F32) + rX1[g, i].astype(F32)).astype(BF)
        for d in (1, 0, 2):
            remote(tX.at[g, ypeer[d]], rX2.at[g, d], ys.at[g, 1], yr.at[g, 1], ylon[d], dp)
        sent.append((rX2.at[g], ys.at[g, 1]))

    def stage_d(g, h):
        if h == 0:
            wait_all(rY2.at[g], xr.at[g, 1])
            v = tYo[g] + rY2[g].astype(F32)
        else:
            wait_all(rX2.at[g], yr.at[g, 1])
            v = tX[g, y].astype(F32)
            for d in range(3):
                v = v + rX2[g, d].astype(F32)
        sC[h, 0:BLOCK] = v
        for u in range(DPS):
            sendD[g, h, u] = sC[h, u * UNIT:u * UNIT + 16].astype(BF)
        for d in FAR_FIRST:
            remote(sendD.at[g, h, dpeer[d]], recvD.at[g, h, d - 1],
                   ds_.at[g, h], dr.at[g, h], lon, dpeer[d])
        sent.append((recvD.at[g, h], ds_.at[g, h]))

    norm = float(16 * LAT * 768) ** -0.5

    def finish(g, h):
        wait_all(recvD.at[g, h], dr.at[g, h])
        v = sendD[g, h, dp].astype(F32)
        for d in range(DPS - 1):
            v = v + recvD[g, h, d].astype(F32)
        v = v * norm
        for u in range(UNIT):
            gbuf[g, pl.ds(u * CH + h * HALF, HALF)] = v[u]

    stage_a(1)
    with scope("inner1"):
        build_inner(V1, PAD1, W1)
    with scope("dx1c"):
        dx_loop(V1, wt1, (1,), blocks1, M1, first1)
    with scope("dw1c"):
        dw(0, xT, V1, cells1, (1,))
    with scope("halo1w"):
        for h in halo1:
            h.wait_recv()
    with scope("edge1"):
        build_edge(V1, PAD1, R1, W1)
    with scope("dw1lr"):
        dw(0, xT, V1, cells1, (0, 2))
    stage_a(0)
    with scope("b2"):
        stage_b(1)
    with scope("dx1lr"):
        dx_loop(V1, wt1, (0, 2), blocks1, M1, last1)
    store = pltpu.make_async_copy(obuf, dx, st.at[0])
    store.start()
    with scope("b1"):
        stage_b(0)
    with scope("c2y"):
        stage_cy(1)
    with scope("c2x"):
        stage_cx(1)
    with scope("c1y"):
        stage_cy(0)
    with scope("c1x"):
        stage_cx(0)
    with scope("know2"):
        pl.semaphore_wait(know2, 1)
    with scope("d2y"):
        stage_d(1, 0)
    with scope("d2x"):
        stage_d(1, 1)
    with scope("d1y"):
        stage_d(0, 0)
    with scope("d1x"):
        stage_d(0, 1)
    with scope("f2"):
        finish(1, 0)
        finish(1, 1)
        put2 = pltpu.make_async_copy(gbuf.at[1], g2, st.at[2])
        put2.start()
    with scope("f1"):
        finish(0, 0)
        finish(0, 1)
        put1 = pltpu.make_async_copy(gbuf.at[0], g1, st.at[1])
        put1.start()
    with scope("sends"):
        for c in halo2 + halo1:
            c.wait_send()
        for ref, sem in sent:
            wait_all(ref, sem)
        store.wait()
        put2.wait()
        put1.wait()


def write_out(dx, g1, g2, dxo, g1o, g2o, dxb, g1b, g2b, rd, wr):
    n = CELLS // 4
    parts = [(dx.at[i * n:(i + 1) * n], dxb.at[i * n:(i + 1) * n], dxo.at[i * n:(i + 1) * n])
             for i in range(4)] + [(g1, g1b, g1o), (g2, g2b, g2o)]
    ins = [pltpu.make_async_copy(s, b, rd.at[i]) for i, (s, b, _) in enumerate(parts)]
    outs = [pltpu.make_async_copy(b, d, wr.at[i]) for i, (_, b, d) in enumerate(parts)]
    for c in ins:
        c.start()
    for c, o in zip(ins, outs):
        c.wait()
        o.start()
    for o in outs:
        o.wait()


def local(inputs, pre_act, cotangent, first_weight, second_weight):
    hbm = pl.BlockSpec(memory_space=pltpu.HBM)
    any_ = pl.BlockSpec(memory_space=pl.ANY)
    V = pltpu.VMEM
    D = pltpu.SemaphoreType.DMA
    outs = (
        jax.ShapeDtypeStruct((CELLS, CH), BF),
        jax.ShapeDtypeStruct((UNIT * CH,), F32),
        jax.ShapeDtypeStruct((UNIT * CH,), F32),
    )
    got = pl.pallas_call(
        kernel,
        name="conv_back",
        out_shape=outs,
        in_specs=[hbm] * 5,
        out_specs=(any_,) * 3,
        scratch_shapes=[
            V((3, CELLS + 2 * PAD2, CH), BF), V((3, CELLS + 2 * PAD1, CH), BF),
            V((2, LAT * W2, CH), BF), V((2, LAT * W2, CH), BF),
            V((2, LAT * W1, CH), BF), V((2, LAT * W1, CH), BF),
            V((CELLS, CH), BF), V((CELLS, CH), BF),
            V((ROWS, CH), BF), V((ROWS, CH), BF),
            V((3, 3 * CH, CH), BF), V((3, 3 * CH, CH), BF),
            V((CH, CELLS), BF), V((CH, CELLS), BF),
            V((CELLS, CH), F32), V((CELLS, CH), BF),
            V((2, ROWS, CH), F32), V((2, ROWS, CH), BF),
            V((2, 8, BLOCK, CH), BF),
            V((2, 2, 4, BLOCK, HALF), BF), V((2, 2, 4, BLOCK, HALF), BF),
            V((2, 3, 2, BLOCK, HALF), BF), V((2, 4, BLOCK, HALF), BF),
            V((2, BLOCK, HALF), BF), V((2, 4, BLOCK, HALF), BF),
            V((2, BLOCK, HALF), BF), V((2, 3, BLOCK, HALF), BF),
            V((2, BLOCK, HALF), F32), V((2, BLOCK + 16, HALF), F32),
            V((2, 2, DPS, 16, HALF), BF), V((2, 2, DPS - 1, 16, HALF), BF), V((2, UNIT * CH), F32),
            D((5,)), D((3,)), D((4,)), D((4,)), D((2,)), D((2,)), D((2, 2)), D((2, 2)),
            D((2, 2)), D((2, 2)), D((2, 2)), D((2, 2)),
            pltpu.SemaphoreType.REGULAR, pltpu.SemaphoreType.REGULAR,
        ],
        compiler_params=pltpu.CompilerParams(
            collective_id=0, has_side_effects=True, vmem_limit_bytes=64300 * 1024),
    )(cotangent.reshape(CELLS, CH), pre_act.reshape(CELLS, CH), inputs.reshape(CELLS, CH),
      first_weight, second_weight)
    dx, g1, g2 = pl.pallas_call(
        write_out,
        name="write_out",
        out_shape=outs,
        in_specs=[any_] * 3,
        out_specs=(any_,) * 3,
        scratch_shapes=[V(o.shape, o.dtype) for o in outs] + [D((6,)), D((6,))],
        compiler_params=pltpu.CompilerParams(vmem_limit_bytes=64300 * 1024),
    )(*got)
    return dx.reshape(inputs.shape), g1, g2


def solution(mesh):
    whole = P("dp", None, "lon", None)
    return jax.shard_map(
        local, mesh=mesh, in_specs=(whole, whole, whole, P(), P()),
        out_specs=(whole, P(("lon", "dp")), P(("lon", "dp"))), check_vma=False)
```

```python
import jax
import jax.numpy as jnp
from jax import lax
from jax.experimental import pallas as pl
from jax.experimental.pallas import tpu as pltpu
from jax.sharding import PartitionSpec as P

BF = jnp.bfloat16
F32 = jnp.float32
LAT = 32
COLS = 48
CH = 256
HALF = 128
CELLS = LAT * COLS
LONS = 16
DPS = 16
ROWS = 9 * CH
BLOCK = ROWS // LONS
UNIT = BLOCK // DPS
PAD2 = 96
TOP = 80
REST = BLOCK - TOP
PAD1 = 64
W2 = 18
W1 = 12
M2 = 384
M1 = 256
MESH = pl.DeviceIdType.MESH
FAR_FIRST = sorted(range(1, DPS), key=lambda d: -min(d, DPS - d))
scope = jax.named_scope


def mm(a, b):
    return jnp.dot(a, b, preferred_element_type=F32)


def kernel(cot, pre2, x2, w1, w2, dx, g1, g2,
           V2, V1, S2, R2, S1, R1, pre, xin, w1b, w2b, wt1, wt2, hT, xT, acc, obuf,
           wf, wb, recvA, sY, sX, rY1, rX1, tY, tX, rY2, rX2, sC, sendD, recvD, gbuf,
           ld, st, hs, hr, as_, ar, ys, yr, xs, xr, ds_, dr, know1, know2):
    lon = lax.axis_index("lon")
    dp = lax.axis_index("dp")
    core = lax.rem(lon, 2)
    y = lax.rem(lax.div(lon, 2), 4)
    xh = lax.div(lon, 8)
    left = lax.rem(lon + LONS - 1, LONS)
    right = lax.rem(lon + 1, LONS)
    partner = lon + 1 - 2 * core
    ypeer = [lax.rem(y + d, 4) for d in range(1, 4)]
    ylon = [xh * 8 + yp * 2 + core for yp in ypeer]
    xl = lax.rem(dp, 2)
    xat = [lax.rem(2 * xh + xl + e, 4) for e in range(1, 4)]
    xpeer = [(lax.div(a, 2), lax.rem(a, 2)) for a in xat]
    xid = [(h * 8 + y * 2 + core, dp - xl + l) for h, l in xpeer]
    dpeer = {d: lax.rem(dp + d, DPS) for d in range(1, DPS)}
    twin = dp + 1 - 2 * lax.rem(dp, 2)

    loads = []
    for i, (s, d) in enumerate((
        (cot, V2.at[1, PAD2:PAD2 + CELLS]), (w2, w2b), (pre2, pre), (x2, xin), (w1, w1b),
    )):
        c = pltpu.make_async_copy(s, d, ld.at[i])
        c.start()
        loads.append(c)

    barrier = pltpu.get_barrier_semaphore()

    def tell(sem, l, d):
        pl.semaphore_signal(sem, inc=1, device_id=(l, d), device_id_type=MESH)

    for l in [left, right] + ylon:
        tell(barrier, l, dp)
    for l, d in xid:
        tell(barrier, l, d)
    for d in (dpeer[2], dpeer[14], dpeer[4], dpeer[12]):
        tell(barrier, lon, d)

    for c in range(3):
        V2[c, 0:PAD2] = jnp.zeros((PAD2, CH), BF)
        V2[c, PAD2 + CELLS:] = jnp.zeros((PAD2, CH), BF)
        V1[c, 0:PAD1] = jnp.zeros((PAD1, CH), BF)
        V1[c, PAD1 + CELLS:] = jnp.zeros((PAD1, CH), BF)
    sC[BLOCK:] = jnp.zeros((16, HALF), F32)

    def remote(s, d, ss, rs, l, dd):
        c = pltpu.make_async_remote_copy(
            src_ref=s, dst_ref=d, send_sem=ss, recv_sem=rs,
            device_id=(l, dd), device_id_type=MESH)
        c.start()
        return c

    def wait_all(ref, sem):
        pltpu.make_async_copy(ref, ref, sem).wait()

    sent = []

    def pack(V, pad, S, w):
        for p in range(LAT):
            o = pad + p * COLS
            S[0, p * w:(p + 1) * w] = V[1, o + COLS - w:o + COLS]
            S[1, p * w:(p + 1) * w] = V[1, o:o + w]

    def build_inner(V, pad, w):
        for p in range(LAT):
            o = pad + p * COLS
            V[0, o:o + COLS - w] = V[1, o + w:o + COLS]
            V[2, o + w:o + COLS] = V[1, o:o + COLS - w]

    early, late = 2 * core, 2 - 2 * core

    def build_edge(V, pad, R, w, i, first):
        wait_all(R.at[1 - core if first else core], hr.at[i + 1 - core if first else i + core])

        @pl.when(core == (0 if first else 1))
        def _():
            for p in range(LAT):
                o = pad + p * COLS
                V[0, o + COLS - w:o + COLS] = R[1, p * w:(p + 1) * w]

        @pl.when(core == (1 if first else 0))
        def _():
            for p in range(LAT):
                o = pad + p * COLS
                V[2, o:o + w] = R[0, p * w:(p + 1) * w]

    def send_halo(S, R, i):
        return [
            remote(S.at[0], R.at[0], hs.at[i], hr.at[i], right, dp),
            remote(S.at[1], R.at[1], hs.at[i + 1], hr.at[i + 1], left, dp),
        ]

    with scope("ld0"):
        loads[0].wait()
    with scope("pack2"):
        pack(V2, PAD2, S2, W2)
    with scope("barrier"):
        pl.semaphore_wait(barrier, 12)
    halo2 = send_halo(S2, R2, 0)
    for d in (dpeer[4], dpeer[12]):
        tell(know1, lon, d)
    with scope("inner2"):
        build_inner(V2, PAD2, W2)

    def tr_weights(w, wt):
        for c in range(3):
            for r in range(3):
                k = 3 * r + c
                wt[c, r * CH:(r + 1) * CH] = w[k * CH:(k + 1) * CH].T

    with scope("trans2"):
        loads[1].wait()
        tr_weights(w2b, wt2)
        loads[2].wait()
        for i in range(6):
            rows = pl.ds(i * CH, CH)
            hT[:, rows] = jnp.maximum(pre[rows], jnp.zeros((CH, CH), BF)).T

    blocks2 = ((0, 768, ((0, 960), (1, 96))), (768, 768, ((1, 864), (2, 0))))
    blocks1 = ((0, 512, ((0, 640), (1, 64))),
               (512, 512, ((0, 1152), (1, 576), (2, 0))),
               (1024, 512, ((1, 1088), (2, 512))))

    def dx_part(V, wt, cols, block, i, m):
        taps = block[2]
        lhs, rhs = [], []
        for c in cols:
            for r, s in taps:
                lhs.append(V[c, pl.ds(pl.multiple_of(s + i * m, 16), m)])
            rhs.append(wt[c, taps[0][0] * CH:(taps[-1][0] + 1) * CH])
        return mm(jnp.concatenate(lhs, axis=1), jnp.concatenate(rhs, axis=0))

    def dx_loop(V, wt, cols, blocks, m, put):
        for b in blocks:
            @pl.loop(0, b[1] // m)
            def _(i, b=b):
                put(pl.multiple_of(b[0] + i * m, m), dx_part(V, wt, cols, b, i, m))

    cells2 = ((0, 768, 960), (0, 1536, 96), (768, 768, 0))
    cells1 = ((0, 1024, 640), (0, 1536, 64), (512, 1024, 0))

    def dw(g, srcT, V, cells, cols):
        for c in cols:
            for r in range(3):
                a, n, s = cells[r]
                v = mm(srcT[:, a:a + n], V[c, s:s + n])
                rows = pl.ds(pl.multiple_of((3 * r + c) * CH, CH), CH)
                wf[g, rows] = v
                wb[g, rows] = v.astype(BF)

    def first2(m0, v):
        acc[pl.ds(m0, M2)] = v

    def more2(m0, v):
        acc[pl.ds(m0, M2)] += v

    def mask2(m0, v):
        rows = pl.ds(m0, M2)
        lg = jnp.where(pre[rows].astype(F32) > 0, acc[rows] + v, 0.0).astype(BF)
        V1[1, pl.ds(pl.multiple_of(PAD1 + m0, 16), M2)] = lg

    def first1(m0, v):
        acc[pl.ds(m0, M1)] = v

    def more1(m0, v):
        acc[pl.ds(m0, M1)] += v

    def last1(m0, v):
        rows = pl.ds(m0, M1)
        obuf[rows] = (acc[rows] + v).astype(BF)

    with scope("dx2c"):
        dx_loop(V2, wt2, (1,), blocks2, M2, first2)
    with scope("dw2c"):
        dw(1, hT, V2, cells2, (1,))
    with scope("know1"):
        pl.semaphore_wait(know1, 2)
        tell(know2, lon, twin)
    with scope("trans1"):
        loads[3].wait()
        for i in range(6):
            rows = pl.ds(i * CH, CH)
            xT[:, rows] = xin[rows].T
        loads[4].wait()
        tr_weights(w1b, wt1)

    with scope("halo2e"):
        build_edge(V2, PAD2, R2, W2, 0, True)
    with scope("dx2e"):
        dx_loop(V2, wt2, (early,), blocks2, M2, more2)
    with scope("dw2e"):
        dw(1, hT, V2, cells2, (early,))
    with scope("halo2l"):
        build_edge(V2, PAD2, R2, W2, 0, False)
    with scope("dx2l"):
        dx_loop(V2, wt2, (late,), blocks2, M2, mask2)
    with scope("pack1"):
        pack(V1, PAD1, S1, W1)
    halo1 = send_halo(S1, R1, 2)
    with scope("dw2l"):
        dw(1, hT, V2, cells2, (late,))

    def stage_a(g):
        for j in range(8):
            rows = pl.ds(pl.multiple_of((2 * j + 1 - core) * BLOCK, 16), BLOCK)
            remote(wb.at[g, rows], recvA.at[g, j], as_.at[g], ar.at[g], partner, dp)
        sent.append((recvA.at[g], as_.at[g]))

    def stage_b(g):
        wait_all(recvA.at[g], ar.at[g])

        @pl.loop(0, 8)
        def _(j):
            rows = pl.ds(pl.multiple_of((2 * j + core) * BLOCK, 16), BLOCK)
            v = (wf[g, rows] + recvA[g, j].astype(F32)).astype(BF)
            h, yy = lax.div(j, 4), lax.rem(j, 4)
            sY[g, h, yy] = v[:TOP]
            sX[g, h, 0, yy] = v[TOP:, :HALF]
            sX[g, h, 1, yy] = v[TOP:, HALF:]

        for e in (1, 0, 2):
            h, l = xpeer[e]
            remote(sX.at[g, h, l], rX1.at[g, e], xs.at[g, 0], xr.at[g, 0], *xid[e])
        for d in (1, 0, 2):
            remote(sY.at[g, :, ypeer[d]], rY1.at[g, d], ys.at[g, 0], yr.at[g, 0], ylon[d], dp)
        sent.extend(((rX1.at[g], xs.at[g, 0]), (rY1.at[g], ys.at[g, 0])))

    def stage_cy(g):
        wait_all(rY1.at[g], yr.at[g, 0])
        for h in range(2):
            v = sY[g, h, y].astype(F32)
            for d in range(3):
                v = v + rY1[g, d, h].astype(F32)
            v = v.astype(BF)
            tY[g, h, 0] = v[:, :HALF]
            tY[g, h, 1] = v[:, HALF:]
        for e in (1, 0, 2):
            h, l = xpeer[e]
            remote(tY.at[g, h, l], rY2.at[g, e], xs.at[g, 1], xr.at[g, 1], *xid[e])
        sent.append((rY2.at[g], xs.at[g, 1]))

    def stage_cx(g):
        wait_all(rX1.at[g], xr.at[g, 0])
        for i in range(4):
            v = sX[g, xh, xl, i].astype(F32)
            for e in range(3):
                v = v + rX1[g, e, i].astype(F32)
            tX[g, i] = v.astype(BF)
        for d in (1, 0, 2):
            remote(tX.at[g, ypeer[d]], rX2.at[g, d], ys.at[g, 1], yr.at[g, 1], ylon[d], dp)
        sent.append((rX2.at[g], ys.at[g, 1]))

    def stage_d(g):
        wait_all(rY2.at[g], xr.at[g, 1])
        v = tY[g, xh, xl].astype(F32)
        for e in range(3):
            v = v + rY2[g, e].astype(F32)
        sC[0:TOP] = v
        wait_all(rX2.at[g], yr.at[g, 1])
        v = tX[g, y].astype(F32)
        for d in range(3):
            v = v + rX2[g, d].astype(F32)
        sC[TOP:BLOCK] = v
        for u in range(DPS):
            sendD[g, u] = sC[u * UNIT:u * UNIT + 16].astype(BF)
        for d in FAR_FIRST:
            remote(sendD.at[g, dpeer[d]], recvD.at[g, d - 1], ds_.at[g], dr.at[g], lon, dpeer[d])
        sent.append((recvD.at[g], ds_.at[g]))

    norm = float(16 * LAT * 768) ** -0.5

    def finish(g):
        wait_all(recvD.at[g], dr.at[g])
        mine = sendD[g, dp].astype(F32)
        for d in range(2, DPS, 2):
            mine = mine + recvD[g, d - 1].astype(F32)
        other = recvD[g, 0].astype(F32)
        for d in range(3, DPS, 2):
            other = other + recvD[g, d - 1].astype(F32)
        for h, v in enumerate((jnp.where(xl == 0, mine, other), jnp.where(xl == 0, other, mine))):
            v = v * norm
            for u in range(UNIT):
                gbuf[g, pl.ds(u * CH + h * HALF, HALF)] = v[u]

    stage_a(1)
    with scope("inner1"):
        build_inner(V1, PAD1, W1)
    with scope("dx1c"):
        dx_loop(V1, wt1, (1,), blocks1, M1, first1)
    with scope("dw1c"):
        dw(0, xT, V1, cells1, (1,))
    with scope("halo1e"):
        build_edge(V1, PAD1, R1, W1, 2, True)
    with scope("dw1e"):
        dw(0, xT, V1, cells1, (early,))
    with scope("dx1e"):
        dx_loop(V1, wt1, (early,), blocks1, M1, more1)
    with scope("halo1l"):
        build_edge(V1, PAD1, R1, W1, 2, False)
    with scope("dw1l"):
        dw(0, xT, V1, cells1, (late,))
    stage_a(0)
    with scope("b2"):
        stage_b(1)
    with scope("dx1l"):
        dx_loop(V1, wt1, (late,), blocks1, M1, last1)
    store = pltpu.make_async_copy(obuf, dx, st.at[0])
    store.start()
    with scope("b1"):
        stage_b(0)
    with scope("c2y"):
        stage_cy(1)
    with scope("c2x"):
        stage_cx(1)
    with scope("c1y"):
        stage_cy(0)
    with scope("c1x"):
        stage_cx(0)
    with scope("know2"):
        pl.semaphore_wait(know2, 1)
    with scope("d2"):
        stage_d(1)
    with scope("d1"):
        stage_d(0)
    with scope("f2"):
        finish(1)
        put2 = pltpu.make_async_copy(gbuf.at[1], g2, st.at[2])
        put2.start()
    with scope("f1"):
        finish(0)
        put1 = pltpu.make_async_copy(gbuf.at[0], g1, st.at[1])
        put1.start()
    with scope("sends"):
        for c in halo2 + halo1:
            c.wait_send()
        for ref, sem in sent:
            wait_all(ref, sem)
        store.wait()
        put2.wait()
        put1.wait()


def write_out(dx, g1, g2, dxo, g1o, g2o, dxb, g1b, g2b, rd, wr):
    n = CELLS // 4
    parts = [(dx.at[i * n:(i + 1) * n], dxb.at[i * n:(i + 1) * n], dxo.at[i * n:(i + 1) * n])
             for i in range(4)] + [(g1, g1b, g1o), (g2, g2b, g2o)]
    ins = [pltpu.make_async_copy(s, b, rd.at[i]) for i, (s, b, _) in enumerate(parts)]
    outs = [pltpu.make_async_copy(b, d, wr.at[i]) for i, (_, b, d) in enumerate(parts)]
    for c in ins:
        c.start()
    for c, o in zip(ins, outs):
        c.wait()
        o.start()
    for o in outs:
        o.wait()


def local(inputs, pre_act, cotangent, first_weight, second_weight):
    hbm = pl.BlockSpec(memory_space=pltpu.HBM)
    any_ = pl.BlockSpec(memory_space=pl.ANY)
    V = pltpu.VMEM
    D = pltpu.SemaphoreType.DMA
    outs = (
        jax.ShapeDtypeStruct((CELLS, CH), BF),
        jax.ShapeDtypeStruct((UNIT * CH,), F32),
        jax.ShapeDtypeStruct((UNIT * CH,), F32),
    )
    got = pl.pallas_call(
        kernel,
        name="conv_back",
        out_shape=outs,
        in_specs=[hbm] * 5,
        out_specs=(any_,) * 3,
        scratch_shapes=[
            V((3, CELLS + 2 * PAD2, CH), BF), V((3, CELLS + 2 * PAD1, CH), BF),
            V((2, LAT * W2, CH), BF), V((2, LAT * W2, CH), BF),
            V((2, LAT * W1, CH), BF), V((2, LAT * W1, CH), BF),
            V((CELLS, CH), BF), V((CELLS, CH), BF),
            V((ROWS, CH), BF), V((ROWS, CH), BF),
            V((3, 3 * CH, CH), BF), V((3, 3 * CH, CH), BF),
            V((CH, CELLS), BF), V((CH, CELLS), BF),
            V((CELLS, CH), F32), V((CELLS, CH), BF),
            V((2, ROWS, CH), F32), V((2, ROWS, CH), BF),
            V((2, 8, BLOCK, CH), BF),
            V((2, 2, 4, TOP, CH), BF), V((2, 2, 2, 4, REST, HALF), BF),
            V((2, 3, 2, TOP, CH), BF), V((2, 3, 4, REST, HALF), BF),
            V((2, 2, 2, TOP, HALF), BF), V((2, 4, REST, HALF), BF),
            V((2, 3, TOP, HALF), BF), V((2, 3, REST, HALF), BF),
            V((BLOCK + 16, HALF), F32),
            V((2, DPS, 16, HALF), BF), V((2, DPS - 1, 16, HALF), BF), V((2, UNIT * CH), F32),
            D((5,)), D((3,)), D((4,)), D((4,)), D((2,)), D((2,)), D((2, 2)), D((2, 2)),
            D((2, 2)), D((2, 2)), D((2,)), D((2,)),
            pltpu.SemaphoreType.REGULAR, pltpu.SemaphoreType.REGULAR,
        ],
        compiler_params=pltpu.CompilerParams(
            collective_id=0, has_side_effects=True, vmem_limit_bytes=64300 * 1024),
    )(cotangent.reshape(CELLS, CH), pre_act.reshape(CELLS, CH), inputs.reshape(CELLS, CH),
      first_weight, second_weight)
    dx, g1, g2 = pl.pallas_call(
        write_out,
        name="write_out",
        out_shape=outs,
        in_specs=[any_] * 3,
        out_specs=(any_,) * 3,
        scratch_shapes=[V(o.shape, o.dtype) for o in outs] + [D((6,)), D((6,))],
        compiler_params=pltpu.CompilerParams(vmem_limit_bytes=64300 * 1024),
    )(*got)
    return dx.reshape(inputs.shape), g1, g2


def solution(mesh):
    whole = P("dp", None, "lon", None)
    return jax.shard_map(
        local, mesh=mesh, in_specs=(whole, whole, whole, P(), P()),
        out_specs=(whole, P(("lon", "dp")), P(("lon", "dp"))), check_vma=False)
```

```python
import jax
import jax.numpy as jnp
from jax import lax
from jax.experimental import pallas as pl
from jax.experimental.pallas import tpu as pltpu
from jax.sharding import PartitionSpec as P

BF = jnp.bfloat16
F32 = jnp.float32
LAT = 32
COLS = 48
CH = 256
HALF = 128
CELLS = LAT * COLS
LONS = 16
DPS = 16
ROWS = 9 * CH
BLOCK = ROWS // LONS
UNIT = BLOCK // DPS
PAD2 = 96
TOP = 80
REST = BLOCK - TOP
PAD1 = 64
W2 = 18
W1 = 12
M2 = 384
M1 = 256
MESH = pl.DeviceIdType.MESH
FAR_FIRST = sorted(range(1, DPS), key=lambda d: -min(d, DPS - d))
scope = jax.named_scope


def mm(a, b):
    return jnp.dot(a, b, preferred_element_type=F32)


def kernel(cot, pre2, x2, w1, w2, dx, g1, g2,
           V2, V1, S2, R2, S1, R1, pre, xin, w1b, w2b, wt1, wt2, hT, xT, acc,
           wf, wb, recvA, sY, sX, rY1, rX1, tY, tX, rY2, rX2, sC, sendD, recvD,
           ld, hs, hr, as_, ar, ys, yr, xs, xr, ds_, dr, know1, know2):
    lon = lax.axis_index("lon")
    dp = lax.axis_index("dp")
    core = lax.rem(lon, 2)
    y = lax.rem(lax.div(lon, 2), 4)
    xh = lax.div(lon, 8)
    left = lax.rem(lon + LONS - 1, LONS)
    right = lax.rem(lon + 1, LONS)
    partner = lon + 1 - 2 * core
    ypeer = [lax.rem(y + d, 4) for d in range(1, 4)]
    ylon = [xh * 8 + yp * 2 + core for yp in ypeer]
    xl = lax.rem(dp, 2)
    xat = [lax.rem(2 * xh + xl + e, 4) for e in range(1, 4)]
    xpeer = [(lax.div(a, 2), lax.rem(a, 2)) for a in xat]
    xid = [(h * 8 + y * 2 + core, dp - xl + l) for h, l in xpeer]
    dpeer = {d: lax.rem(dp + d, DPS) for d in range(1, DPS)}
    twin = dp + 1 - 2 * lax.rem(dp, 2)

    loads = []
    for i, (s, d) in enumerate((
        (cot, V2.at[1, PAD2:PAD2 + CELLS]), (w2, w2b), (pre2, pre), (x2, xin), (w1, w1b),
    )):
        c = pltpu.make_async_copy(s, d, ld.at[i])
        c.start()
        loads.append(c)

    barrier = pltpu.get_barrier_semaphore()

    def tell(sem, l, d):
        pl.semaphore_signal(sem, inc=1, device_id=(l, d), device_id_type=MESH)

    for l in [left, right] + ylon:
        tell(barrier, l, dp)
    for l, d in xid:
        tell(barrier, l, d)
    for d in (dpeer[2], dpeer[14], dpeer[4], dpeer[12]):
        tell(barrier, lon, d)

    for c in range(3):
        V2[c, 0:PAD2] = jnp.zeros((PAD2, CH), BF)
        V2[c, PAD2 + CELLS:] = jnp.zeros((PAD2, CH), BF)
        V1[c, 0:PAD1] = jnp.zeros((PAD1, CH), BF)
        V1[c, PAD1 + CELLS:] = jnp.zeros((PAD1, CH), BF)
    sC[BLOCK:] = jnp.zeros((16, HALF), F32)

    def remote(s, d, ss, rs, l, dd):
        c = pltpu.make_async_remote_copy(
            src_ref=s, dst_ref=d, send_sem=ss, recv_sem=rs,
            device_id=(l, dd), device_id_type=MESH)
        c.start()
        return c

    def wait_all(ref, sem):
        pltpu.make_async_copy(ref, ref, sem).wait()

    sent = []

    def pack(V, pad, S, w):
        for p in range(LAT):
            o = pad + p * COLS
            S[0, p * w:(p + 1) * w] = V[1, o + COLS - w:o + COLS]
            S[1, p * w:(p + 1) * w] = V[1, o:o + w]

    def build_inner(V, pad, w):
        for p in range(LAT):
            o = pad + p * COLS
            V[0, o:o + COLS - w] = V[1, o + w:o + COLS]
            V[2, o + w:o + COLS] = V[1, o:o + COLS - w]

    early, late = 2 * core, 2 - 2 * core

    def build_edge(V, pad, R, w, i, first):
        wait_all(R.at[1 - core if first else core], hr.at[i + 1 - core if first else i + core])

        @pl.when(core == (0 if first else 1))
        def _():
            for p in range(LAT):
                o = pad + p * COLS
                V[0, o + COLS - w:o + COLS] = R[1, p * w:(p + 1) * w]

        @pl.when(core == (1 if first else 0))
        def _():
            for p in range(LAT):
                o = pad + p * COLS
                V[2, o:o + w] = R[0, p * w:(p + 1) * w]

    def send_halo(S, R, i):
        return [
            remote(S.at[0], R.at[0], hs.at[i], hr.at[i], right, dp),
            remote(S.at[1], R.at[1], hs.at[i + 1], hr.at[i + 1], left, dp),
        ]

    with scope("ld0"):
        loads[0].wait()
    with scope("pack2"):
        pack(V2, PAD2, S2, W2)
    with scope("barrier"):
        pl.semaphore_wait(barrier, 12)
    halo2 = send_halo(S2, R2, 0)
    for d in (dpeer[4], dpeer[12]):
        tell(know1, lon, d)
    with scope("inner2"):
        build_inner(V2, PAD2, W2)

    def tr_weights(w, wt):
        for c in range(3):
            for r in range(3):
                k = 3 * r + c
                wt[c, r * CH:(r + 1) * CH] = w[k * CH:(k + 1) * CH].T

    with scope("trans2"):
        loads[1].wait()
        tr_weights(w2b, wt2)
        loads[2].wait()
        for i in range(6):
            rows = pl.ds(i * CH, CH)
            hT[:, rows] = jnp.maximum(pre[rows], jnp.zeros((CH, CH), BF)).T

    blocks2 = ((0, 768, ((0, 960), (1, 96))), (768, 768, ((1, 864), (2, 0))))
    blocks1 = ((0, 512, ((0, 640), (1, 64))),
               (512, 512, ((0, 1152), (1, 576), (2, 0))),
               (1024, 512, ((1, 1088), (2, 512))))

    def dx_part(V, wt, cols, block, i, m):
        taps = block[2]
        lhs, rhs = [], []
        for c in cols:
            for r, s in taps:
                lhs.append(V[c, pl.ds(pl.multiple_of(s + i * m, 16), m)])
            rhs.append(wt[c, taps[0][0] * CH:(taps[-1][0] + 1) * CH])
        return mm(jnp.concatenate(lhs, axis=1), jnp.concatenate(rhs, axis=0))

    def dx_loop(V, wt, cols, blocks, m, put):
        for b in blocks:
            @pl.loop(0, b[1] // m)
            def _(i, b=b):
                put(pl.multiple_of(b[0] + i * m, m), dx_part(V, wt, cols, b, i, m))

    cells2 = ((0, 768, 960), (0, 1536, 96), (768, 768, 0))
    cells1 = ((0, 1024, 640), (0, 1536, 64), (512, 1024, 0))

    def dw(g, srcT, V, cells, cols):
        for c in cols:
            for r in range(3):
                a, n, s = cells[r]
                v = mm(srcT[:, a:a + n], V[c, s:s + n])
                rows = pl.ds(pl.multiple_of((3 * r + c) * CH, CH), CH)
                wf[g, rows] = v
                wb[g, rows] = v.astype(BF)

    def first2(m0, v):
        acc[pl.ds(m0, M2)] = v

    def more2(m0, v):
        acc[pl.ds(m0, M2)] += v

    def mask2(m0, v):
        rows = pl.ds(m0, M2)
        lg = jnp.where(pre[rows].astype(F32) > 0, acc[rows] + v, 0.0).astype(BF)
        V1[1, pl.ds(pl.multiple_of(PAD1 + m0, 16), M2)] = lg

    def first1(m0, v):
        acc[pl.ds(m0, M1)] = v

    def more1(m0, v):
        acc[pl.ds(m0, M1)] += v

    def last1(m0, v):
        rows = pl.ds(m0, M1)
        dx[rows] = (acc[rows] + v).astype(BF)

    with scope("dx2c"):
        dx_loop(V2, wt2, (1,), blocks2, M2, first2)
    with scope("dw2c"):
        dw(1, hT, V2, cells2, (1,))
    with scope("know1"):
        pl.semaphore_wait(know1, 2)
        tell(know2, lon, twin)
    with scope("trans1"):
        loads[3].wait()
        for i in range(6):
            rows = pl.ds(i * CH, CH)
            xT[:, rows] = xin[rows].T
        loads[4].wait()
        tr_weights(w1b, wt1)

    with scope("halo2e"):
        build_edge(V2, PAD2, R2, W2, 0, True)
    with scope("dx2e"):
        dx_loop(V2, wt2, (early,), blocks2, M2, more2)
    with scope("dw2e"):
        dw(1, hT, V2, cells2, (early,))
    with scope("halo2l"):
        build_edge(V2, PAD2, R2, W2, 0, False)
    with scope("dx2l"):
        dx_loop(V2, wt2, (late,), blocks2, M2, mask2)
    with scope("pack1"):
        pack(V1, PAD1, S1, W1)
    halo1 = send_halo(S1, R1, 2)
    with scope("dw2l"):
        dw(1, hT, V2, cells2, (late,))

    def stage_a(g):
        for j in range(8):
            rows = pl.ds(pl.multiple_of((2 * j + 1 - core) * BLOCK, 16), BLOCK)
            remote(wb.at[g, rows], recvA.at[g, j], as_.at[g], ar.at[g], partner, dp)
        sent.append((recvA.at[g], as_.at[g]))

    def stage_b(g):
        wait_all(recvA.at[g], ar.at[g])

        @pl.loop(0, 8)
        def _(j):
            rows = pl.ds(pl.multiple_of((2 * j + core) * BLOCK, 16), BLOCK)
            v = (wf[g, rows] + recvA[g, j].astype(F32)).astype(BF)
            h, yy = lax.div(j, 4), lax.rem(j, 4)
            sY[g, h, yy] = v[:TOP]
            sX[g, h, 0, yy] = v[TOP:, :HALF]
            sX[g, h, 1, yy] = v[TOP:, HALF:]

        for e in (1, 0, 2):
            h, l = xpeer[e]
            remote(sX.at[g, h, l], rX1.at[g, e], xs.at[g, 0], xr.at[g, 0], *xid[e])
        for d in (1, 0, 2):
            remote(sY.at[g, :, ypeer[d]], rY1.at[g, d], ys.at[g, 0], yr.at[g, 0], ylon[d], dp)
        sent.extend(((rX1.at[g], xs.at[g, 0]), (rY1.at[g], ys.at[g, 0])))

    def stage_cy(g):
        wait_all(rY1.at[g], yr.at[g, 0])
        for h in range(2):
            v = sY[g, h, y].astype(F32)
            for d in range(3):
                v = v + rY1[g, d, h].astype(F32)
            v = v.astype(BF)
            tY[g, h, 0] = v[:, :HALF]
            tY[g, h, 1] = v[:, HALF:]
        for e in (1, 0, 2):
            h, l = xpeer[e]
            remote(tY.at[g, h, l], rY2.at[g, e], xs.at[g, 1], xr.at[g, 1], *xid[e])
        sent.append((rY2.at[g], xs.at[g, 1]))

    def stage_cx(g):
        wait_all(rX1.at[g], xr.at[g, 0])
        for i in range(4):
            v = sX[g, xh, xl, i].astype(F32)
            for e in range(3):
                v = v + rX1[g, e, i].astype(F32)
            tX[g, i] = v.astype(BF)
        for d in (1, 0, 2):
            remote(tX.at[g, ypeer[d]], rX2.at[g, d], ys.at[g, 1], yr.at[g, 1], ylon[d], dp)
        sent.append((rX2.at[g], ys.at[g, 1]))

    def stage_d(g):
        wait_all(rY2.at[g], xr.at[g, 1])
        v = tY[g, xh, xl].astype(F32)
        for e in range(3):
            v = v + rY2[g, e].astype(F32)
        sC[0:TOP] = v
        wait_all(rX2.at[g], yr.at[g, 1])
        v = tX[g, y].astype(F32)
        for d in range(3):
            v = v + rX2[g, d].astype(F32)
        sC[TOP:BLOCK] = v
        for u in range(DPS):
            sendD[g, u] = sC[u * UNIT:u * UNIT + 16].astype(BF)
        for d in FAR_FIRST:
            remote(sendD.at[g, dpeer[d]], recvD.at[g, d - 1], ds_.at[g], dr.at[g], lon, dpeer[d])
        sent.append((recvD.at[g], ds_.at[g]))

    norm = float(16 * LAT * 768) ** -0.5

    def finish(g, out):
        wait_all(recvD.at[g], dr.at[g])
        mine = sendD[g, dp].astype(F32)
        for d in range(2, DPS, 2):
            mine = mine + recvD[g, d - 1].astype(F32)
        other = recvD[g, 0].astype(F32)
        for d in range(3, DPS, 2):
            other = other + recvD[g, d - 1].astype(F32)
        for h, v in enumerate((jnp.where(xl == 0, mine, other), jnp.where(xl == 0, other, mine))):
            v = v * norm
            for u in range(UNIT):
                out[pl.ds(u * CH + h * HALF, HALF)] = v[u]

    stage_a(1)
    with scope("inner1"):
        build_inner(V1, PAD1, W1)
    with scope("dx1c"):
        dx_loop(V1, wt1, (1,), blocks1, M1, first1)
    with scope("dw1c"):
        dw(0, xT, V1, cells1, (1,))
    with scope("halo1e"):
        build_edge(V1, PAD1, R1, W1, 2, True)
    with scope("dw1e"):
        dw(0, xT, V1, cells1, (early,))
    with scope("dx1e"):
        dx_loop(V1, wt1, (early,), blocks1, M1, more1)
    with scope("halo1l"):
        build_edge(V1, PAD1, R1, W1, 2, False)
    with scope("dw1l"):
        dw(0, xT, V1, cells1, (late,))
    stage_a(0)
    with scope("b2"):
        stage_b(1)
    with scope("dx1l"):
        dx_loop(V1, wt1, (late,), blocks1, M1, last1)
    with scope("b1"):
        stage_b(0)
    with scope("c2y"):
        stage_cy(1)
    with scope("c2x"):
        stage_cx(1)
    with scope("c1y"):
        stage_cy(0)
    with scope("c1x"):
        stage_cx(0)
    with scope("know2"):
        pl.semaphore_wait(know2, 1)
    with scope("d2"):
        stage_d(1)
    with scope("d1"):
        stage_d(0)
    with scope("f2"):
        finish(1, g2)
    with scope("f1"):
        finish(0, g1)
    with scope("sends"):
        for c in halo2 + halo1:
            c.wait_send()
        for ref, sem in sent:
            wait_all(ref, sem)


def write_out(dx, g1, g2, dxo, g1o, g2o, sem):
    copies = [pltpu.make_async_copy(s, d, sem.at[i])
              for i, (s, d) in enumerate(((g1, g1o), (g2, g2o), (dx, dxo)))]
    for c in copies:
        c.start()
    for c in copies:
        c.wait()


def local(inputs, pre_act, cotangent, first_weight, second_weight):
    hbm = pl.BlockSpec(memory_space=pltpu.HBM)
    vm = pl.BlockSpec(memory_space=pltpu.VMEM)
    any_ = pl.BlockSpec(memory_space=pl.ANY)
    V = pltpu.VMEM
    D = pltpu.SemaphoreType.DMA
    outs = (
        jax.ShapeDtypeStruct((CELLS, CH), BF),
        jax.ShapeDtypeStruct((UNIT * CH,), F32),
        jax.ShapeDtypeStruct((UNIT * CH,), F32),
    )
    got = pl.pallas_call(
        kernel,
        name="conv_back",
        out_shape=outs,
        in_specs=[hbm] * 5,
        out_specs=(vm,) * 3,
        scratch_shapes=[
            V((3, CELLS + 2 * PAD2, CH), BF), V((3, CELLS + 2 * PAD1, CH), BF),
            V((2, LAT * W2, CH), BF), V((2, LAT * W2, CH), BF),
            V((2, LAT * W1, CH), BF), V((2, LAT * W1, CH), BF),
            V((CELLS, CH), BF), V((CELLS, CH), BF),
            V((ROWS, CH), BF), V((ROWS, CH), BF),
            V((3, 3 * CH, CH), BF), V((3, 3 * CH, CH), BF),
            V((CH, CELLS), BF), V((CH, CELLS), BF),
            V((CELLS, CH), F32),
            V((2, ROWS, CH), F32), V((2, ROWS, CH), BF),
            V((2, 8, BLOCK, CH), BF),
            V((2, 2, 4, TOP, CH), BF), V((2, 2, 2, 4, REST, HALF), BF),
            V((2, 3, 2, TOP, CH), BF), V((2, 3, 4, REST, HALF), BF),
            V((2, 2, 2, TOP, HALF), BF), V((2, 4, REST, HALF), BF),
            V((2, 3, TOP, HALF), BF), V((2, 3, REST, HALF), BF),
            V((BLOCK + 16, HALF), F32),
            V((2, DPS, 16, HALF), BF), V((2, DPS - 1, 16, HALF), BF),
            D((5,)), D((4,)), D((4,)), D((2,)), D((2,)), D((2, 2)), D((2, 2)),
            D((2, 2)), D((2, 2)), D((2,)), D((2,)),
            pltpu.SemaphoreType.REGULAR, pltpu.SemaphoreType.REGULAR,
        ],
        compiler_params=pltpu.CompilerParams(
            collective_id=0, has_side_effects=True, vmem_limit_bytes=53760 * 1024),
    )(cotangent.reshape(CELLS, CH), pre_act.reshape(CELLS, CH), inputs.reshape(CELLS, CH),
      first_weight, second_weight)
    dx, g1, g2 = pl.pallas_call(
        write_out,
        name="write_out",
        out_shape=outs,
        in_specs=[vm] * 3,
        out_specs=(any_,) * 3,
        scratch_shapes=[D((3,))],
        compiler_params=pltpu.CompilerParams(vmem_limit_bytes=1024 * 1024),
    )(*got)
    return dx.reshape(inputs.shape), g1, g2


def solution(mesh):
    whole = P("dp", None, "lon", None)
    return jax.shard_map(
        local, mesh=mesh, in_specs=(whole, whole, whole, P(), P()),
        out_specs=(whole, P(("lon", "dp")), P(("lon", "dp"))), check_vma=False)
```

```python
import jax
import jax.numpy as jnp
from jax import lax
from jax.experimental import pallas as pl
from jax.experimental.pallas import tpu as pltpu
from jax.sharding import PartitionSpec as P

BF = jnp.bfloat16
F32 = jnp.float32
LAT = 32
COLS = 48
CH = 256
HALF = 128
CELLS = LAT * COLS
LONS = 16
DPS = 16
ROWS = 9 * CH
BLOCK = ROWS // LONS
UNIT = BLOCK // DPS
PAD2 = 96
TOP = 64
REST = BLOCK - TOP
PAD1 = 64
W2 = 18
W1 = 12
M2 = 384
M1 = 256
MESH = pl.DeviceIdType.MESH
FAR_FIRST = sorted(range(1, DPS), key=lambda d: -min(d, DPS - d))
scope = jax.named_scope


def mm(a, b):
    return jnp.dot(a, b, preferred_element_type=F32)


def kernel(cot, pre2, x2, w1, w2, dx, g1, g2,
           V2, V1, S2, R2, S1, R1, pre, xin, w1b, w2b, wt1, wt2, hT, xT, acc,
           wf, wb, recvA, sY, sX, rY1, rX1, tY, tX, rY2, rX2, sC, sendD, recvD,
           ld, hs, hr, as_, ar, ys, yr, xs, xr, ds_, dr, know1, know2):
    lon = lax.axis_index("lon")
    dp = lax.axis_index("dp")
    core = lax.rem(lon, 2)
    y = lax.rem(lax.div(lon, 2), 4)
    xh = lax.div(lon, 8)
    left = lax.rem(lon + LONS - 1, LONS)
    right = lax.rem(lon + 1, LONS)
    partner = lon + 1 - 2 * core
    ypeer = [lax.rem(y + d, 4) for d in range(1, 4)]
    ylon = [xh * 8 + yp * 2 + core for yp in ypeer]
    xl = lax.rem(dp, 2)
    xat = [lax.rem(2 * xh + xl + e, 4) for e in range(1, 4)]
    xpeer = [(lax.div(a, 2), lax.rem(a, 2)) for a in xat]
    xid = [(h * 8 + y * 2 + core, dp - xl + l) for h, l in xpeer]
    dpeer = {d: lax.rem(dp + d, DPS) for d in range(1, DPS)}
    twin = dp + 1 - 2 * lax.rem(dp, 2)

    loads = []
    for i, (s, d) in enumerate((
        (cot, V2.at[1, PAD2:PAD2 + CELLS]), (w2, w2b), (pre2, pre), (x2, xin), (w1, w1b),
    )):
        c = pltpu.make_async_copy(s, d, ld.at[i])
        c.start()
        loads.append(c)

    barrier = pltpu.get_barrier_semaphore()

    def tell(sem, l, d):
        pl.semaphore_signal(sem, inc=1, device_id=(l, d), device_id_type=MESH)

    for l in [left, right] + ylon:
        tell(barrier, l, dp)
    for l, d in xid:
        tell(barrier, l, d)
    for d in (dpeer[2], dpeer[14], dpeer[4], dpeer[12]):
        tell(barrier, lon, d)

    for c in range(3):
        V2[c, 0:PAD2] = jnp.zeros((PAD2, CH), BF)
        V2[c, PAD2 + CELLS:] = jnp.zeros((PAD2, CH), BF)
        V1[c, 0:PAD1] = jnp.zeros((PAD1, CH), BF)
        V1[c, PAD1 + CELLS:] = jnp.zeros((PAD1, CH), BF)
    sC[BLOCK:] = jnp.zeros((16, HALF), F32)

    def remote(s, d, ss, rs, l, dd):
        c = pltpu.make_async_remote_copy(
            src_ref=s, dst_ref=d, send_sem=ss, recv_sem=rs,
            device_id=(l, dd), device_id_type=MESH)
        c.start()
        return c

    def wait_all(ref, sem):
        pltpu.make_async_copy(ref, ref, sem).wait()

    sent = []

    halves = (range(0, LAT // 2), range(LAT // 2, LAT))

    def pack(V, pad, S, w, lats=range(LAT)):
        for p in lats:
            o = pad + p * COLS
            S[0, p * w:(p + 1) * w] = V[1, o + COLS - w:o + COLS]
            S[1, p * w:(p + 1) * w] = V[1, o:o + w]

    def build_inner(V, pad, w):
        for p in range(LAT):
            o = pad + p * COLS
            V[0, o:o + COLS - w] = V[1, o + w:o + COLS]
            V[2, o + w:o + COLS] = V[1, o:o + COLS - w]

    early, late = 2 * core, 2 - 2 * core

    def build_edge(V, pad, R, w, i, first, q):
        n = LAT // 2 * w
        wait_all(R.at[1 - core if first else core, q * n:(q + 1) * n],
                 hr.at[i, 1 - core if first else core, q])

        @pl.when(core == (0 if first else 1))
        def _():
            for p in halves[q]:
                o = pad + p * COLS
                V[0, o + COLS - w:o + COLS] = R[1, p * w:(p + 1) * w]

        @pl.when(core == (1 if first else 0))
        def _():
            for p in halves[q]:
                o = pad + p * COLS
                V[2, o:o + w] = R[0, p * w:(p + 1) * w]

    def send_halo(S, R, i, q):
        n = S.shape[1] // 2
        rows = slice(q * n, (q + 1) * n)
        remote(S.at[0, rows], R.at[0, rows], hs.at[i, 0], hr.at[i, 0, q], right, dp)
        remote(S.at[1, rows], R.at[1, rows], hs.at[i, 1], hr.at[i, 1, q], left, dp)
        if q:
            sent.extend(((R.at[0], hs.at[i, 0]), (R.at[1], hs.at[i, 1])))

    with scope("ld0"):
        loads[0].wait()
    with scope("pack2"):
        pack(V2, PAD2, S2, W2)
    with scope("barrier"):
        pl.semaphore_wait(barrier, 12)
    for q in range(2):
        send_halo(S2, R2, 0, q)
    for d in (dpeer[4], dpeer[12]):
        tell(know1, lon, d)
    with scope("inner2"):
        build_inner(V2, PAD2, W2)

    def tr_weights(w, wt):
        for c in range(3):
            for r in range(3):
                k = 3 * r + c
                wt[c, r * CH:(r + 1) * CH] = w[k * CH:(k + 1) * CH].T

    with scope("trans2"):
        loads[1].wait()
        tr_weights(w2b, wt2)
        loads[2].wait()
        for i in range(6):
            rows = pl.ds(i * CH, CH)
            hT[:, rows] = jnp.maximum(pre[rows], jnp.zeros((CH, CH), BF)).T

    blocks2 = ((0, 768, ((0, 960), (1, 96))), (768, 768, ((1, 864), (2, 0))))
    blocks1 = ((0, 512, ((0, 640), (1, 64))),
               (512, 512, ((0, 1152), (1, 576), (2, 0))),
               (1024, 512, ((1, 1088), (2, 512))))

    def dx_part(V, wt, cols, block, i, m):
        taps = block[2]
        lhs, rhs = [], []
        for c in cols:
            for r, s in taps:
                lhs.append(V[c, pl.ds(pl.multiple_of(s + i * m, 16), m)])
            rhs.append(wt[c, taps[0][0] * CH:(taps[-1][0] + 1) * CH])
        return mm(jnp.concatenate(lhs, axis=1), jnp.concatenate(rhs, axis=0))

    def dx_loop(V, wt, cols, blocks, m, put):
        for b in blocks:
            @pl.loop(0, b[1] // m)
            def _(i, b=b):
                put(pl.multiple_of(b[0] + i * m, m), dx_part(V, wt, cols, b, i, m))

    cells2 = ((0, 768, 960), (0, 1536, 96), (768, 768, 0))
    cells1 = ((0, 1024, 640), (0, 1536, 64), (512, 1024, 0))

    def dw(g, srcT, V, cells, cols):
        for c in cols:
            for r in range(3):
                a, n, s = cells[r]
                v = mm(srcT[:, a:a + n], V[c, s:s + n])
                rows = pl.ds(pl.multiple_of((3 * r + c) * CH, CH), CH)
                wf[g, rows] = v
                wb[g, rows] = v.astype(BF)

    def dw_part(cells, last):
        for r in range(3):
            a, n, s = cells[r]
            v = mm(xT[:, a:a + n], V1[late, s:s + n])
            rows = pl.ds(pl.multiple_of((3 * r + late) * CH, CH), CH)
            if last:
                v = v + wf[0, rows]
                wb[0, rows] = v.astype(BF)
            wf[0, rows] = v

    def first2(m0, v):
        acc[pl.ds(m0, M2)] = v

    def more2(m0, v):
        acc[pl.ds(m0, M2)] += v

    def mask2(m0, v):
        rows = pl.ds(m0, M2)
        lg = jnp.where(pre[rows].astype(F32) > 0, acc[rows] + v, 0.0).astype(BF)
        V1[1, pl.ds(pl.multiple_of(PAD1 + m0, 16), M2)] = lg

    def first1(m0, v):
        acc[pl.ds(m0, M1)] = v

    def more1(m0, v):
        acc[pl.ds(m0, M1)] += v

    def only1(m0, v):
        dx[pl.ds(m0, M1)] = v.astype(BF)

    def last1(m0, v):
        rows = pl.ds(m0, M1)
        dx[rows] = (acc[rows] + v).astype(BF)

    with scope("dx2c"):
        dx_loop(V2, wt2, (1,), blocks2, M2, first2)
    with scope("dw2c"):
        dw(1, hT, V2, cells2, (1,))
    with scope("know1"):
        pl.semaphore_wait(know1, 2)
        tell(know2, lon, twin)
    with scope("trans1"):
        loads[3].wait()
        for i in range(6):
            rows = pl.ds(i * CH, CH)
            xT[:, rows] = xin[rows].T
        loads[4].wait()
        tr_weights(w1b, wt1)

    with scope("halo2e"):
        for q in range(2):
            build_edge(V2, PAD2, R2, W2, 0, True, q)
    with scope("dx2e"):
        dx_loop(V2, wt2, (early,), blocks2, M2, more2)
    with scope("dw2e"):
        dw(1, hT, V2, cells2, (early,))
    with scope("halo2l"):
        build_edge(V2, PAD2, R2, W2, 0, False, 0)
    with scope("dx2l"):
        dx_loop(V2, wt2, (late,), ((0, 768, ((1, 96),)), (768, 768, ((2, 0),))), M2, more2)
    with scope("halo2m"):
        build_edge(V2, PAD2, R2, W2, 0, False, 1)
    for q, b in enumerate(((0, 768, ((0, 960),)), (768, 768, ((1, 864),)))):
        with scope("dx2m%d" % q):
            dx_loop(V2, wt2, (late,), (b,), M2, mask2)
        with scope("pack1%d" % q):
            pack(V1, PAD1, S1, W1, halves[q])
        send_halo(S1, R1, 1, q)
    with scope("dw2l"):
        dw(1, hT, V2, cells2, (late,))

    def stage_a(g):
        for j in range(8):
            rows = pl.ds(pl.multiple_of((2 * j + 1 - core) * BLOCK, 16), BLOCK)
            remote(wb.at[g, rows], recvA.at[g, j], as_.at[g], ar.at[g], partner, dp)
        sent.append((recvA.at[g], as_.at[g]))

    def send_taps(ready):
        for v in range(2):
            @pl.when(core == v)
            def _(v=v):
                for c in (1, 2 * v) if ready else (2 - 2 * v,):
                    for k in (c, 3 + c, 6 + c):
                        for b in range(1 - v, LONS, 2):
                            lo, hi = max(k * CH, b * BLOCK), min((k + 1) * CH, (b + 1) * BLOCK)
                            if lo < hi:
                                remote(wb.at[0, lo:hi], recvA.at[0, b // 2, lo - b * BLOCK:hi - b * BLOCK],
                                       as_.at[0], ar.at[0], partner, dp)

    def stage_b(g):
        wait_all(recvA.at[g], ar.at[g])

        @pl.loop(0, 8)
        def _(j):
            rows = pl.ds(pl.multiple_of((2 * j + core) * BLOCK, 16), BLOCK)
            v = (wf[g, rows] + recvA[g, j].astype(F32)).astype(BF)
            h, yy = lax.div(j, 4), lax.rem(j, 4)
            sY[g, h, yy] = v[:TOP]
            sX[g, h, 0, yy] = v[TOP:, :HALF]
            sX[g, h, 1, yy] = v[TOP:, HALF:]

        for e in (1, 0, 2):
            h, l = xpeer[e]
            remote(sX.at[g, h, l], rX1.at[g, e], xs.at[g, 0], xr.at[g, 0], *xid[e])
        for d in (1, 0, 2):
            remote(sY.at[g, :, ypeer[d]], rY1.at[g, d], ys.at[g, 0], yr.at[g, 0], ylon[d], dp)
        sent.extend(((rX1.at[g], xs.at[g, 0]), (rY1.at[g], ys.at[g, 0])))

    def stage_cy(g):
        wait_all(rY1.at[g], yr.at[g, 0])
        for h in range(2):
            v = sY[g, h, y].astype(F32)
            for d in range(3):
                v = v + rY1[g, d, h].astype(F32)
            v = v.astype(BF)
            tY[g, h, 0] = v[:, :HALF]
            tY[g, h, 1] = v[:, HALF:]
        for e in (1, 0, 2):
            h, l = xpeer[e]
            remote(tY.at[g, h, l], rY2.at[g, e], xs.at[g, 1], xr.at[g, 1], *xid[e])
        sent.append((rY2.at[g], xs.at[g, 1]))

    def stage_cx(g):
        wait_all(rX1.at[g], xr.at[g, 0])
        for i in range(4):
            v = sX[g, xh, xl, i].astype(F32)
            for e in range(3):
                v = v + rX1[g, e, i].astype(F32)
            tX[g, i] = v.astype(BF)
        for d in (1, 0, 2):
            remote(tX.at[g, ypeer[d]], rX2.at[g, d], ys.at[g, 1], yr.at[g, 1], ylon[d], dp)
        sent.append((rX2.at[g], ys.at[g, 1]))

    def stage_d(g):
        wait_all(rY2.at[g], xr.at[g, 1])
        v = tY[g, xh, xl].astype(F32)
        for e in range(3):
            v = v + rY2[g, e].astype(F32)
        sC[0:TOP] = v
        wait_all(rX2.at[g], yr.at[g, 1])
        v = tX[g, y].astype(F32)
        for d in range(3):
            v = v + rX2[g, d].astype(F32)
        sC[TOP:BLOCK] = v
        for u in range(DPS):
            sendD[g, u] = sC[u * UNIT:u * UNIT + 16].astype(BF)
        for d in FAR_FIRST:
            remote(sendD.at[g, dpeer[d]], recvD.at[g, d - 1], ds_.at[g], dr.at[g], lon, dpeer[d])
        sent.append((recvD.at[g], ds_.at[g]))

    norm = float(16 * LAT * 768) ** -0.5

    def finish(g, out):
        wait_all(recvD.at[g], dr.at[g])
        mine = sendD[g, dp].astype(F32)
        for d in range(2, DPS, 2):
            mine = mine + recvD[g, d - 1].astype(F32)
        other = recvD[g, 0].astype(F32)
        for d in range(3, DPS, 2):
            other = other + recvD[g, d - 1].astype(F32)
        for h, v in enumerate((jnp.where(xl == 0, mine, other), jnp.where(xl == 0, other, mine))):
            v = v * norm
            for u in range(UNIT):
                out[pl.ds(u * CH + h * HALF, HALF)] = v[u]

    stage_a(1)
    with scope("inner1"):
        build_inner(V1, PAD1, W1)
    with scope("dw1c"):
        dw(0, xT, V1, cells1, (1,))
    with scope("halo1e"):
        for q in range(2):
            build_edge(V1, PAD1, R1, W1, 1, True, q)
    with scope("dw1e"):
        dw(0, xT, V1, cells1, (early,))
    send_taps(True)
    with scope("halo1l"):
        build_edge(V1, PAD1, R1, W1, 1, False, 0)
    with scope("dw1l"):
        dw_part(((0, 128, 640), (0, 768, 64), (512, 768, 0)), False)
    with scope("halo1m"):
        build_edge(V1, PAD1, R1, W1, 1, False, 1)
    with scope("dw1m"):
        dw_part(((128, 896, 768), (768, 768, 832), (1280, 256, 768)), True)
    send_taps(False)
    sent.append((recvA.at[0], as_.at[0]))
    with scope("b2"):
        stage_b(1)
    with scope("dx1a"):
        dx_loop(V1, wt1, (0, 1, 2), blocks1[:2], M1, only1)
    with scope("b1"):
        stage_b(0)
    with scope("dx1b"):
        dx_loop(V1, wt1, (0, 1, 2), blocks1[2:], M1, only1)
    with scope("c2y"):
        stage_cy(1)
    with scope("c2x"):
        stage_cx(1)
    with scope("c1y"):
        stage_cy(0)
    with scope("c1x"):
        stage_cx(0)
    with scope("know2"):
        pl.semaphore_wait(know2, 1)
    with scope("d2"):
        stage_d(1)
    with scope("d1"):
        stage_d(0)
    with scope("f2"):
        finish(1, g2)
    with scope("f1"):
        finish(0, g1)
    with scope("sends"):
        for ref, sem in sent:
            wait_all(ref, sem)


def write_out(dx, g1, g2, dxo, g1o, g2o, sem):
    copies = [pltpu.make_async_copy(s, d, sem.at[i])
              for i, (s, d) in enumerate(((g1, g1o), (g2, g2o), (dx, dxo)))]
    for c in copies:
        c.start()
    for c in copies:
        c.wait()


def local(inputs, pre_act, cotangent, first_weight, second_weight):
    hbm = pl.BlockSpec(memory_space=pltpu.HBM)
    vm = pl.BlockSpec(memory_space=pltpu.VMEM)
    any_ = pl.BlockSpec(memory_space=pl.ANY)
    V = pltpu.VMEM
    D = pltpu.SemaphoreType.DMA
    outs = (
        jax.ShapeDtypeStruct((CELLS, CH), BF),
        jax.ShapeDtypeStruct((UNIT * CH,), F32),
        jax.ShapeDtypeStruct((UNIT * CH,), F32),
    )
    got = pl.pallas_call(
        kernel,
        name="conv_back",
        out_shape=outs,
        in_specs=[hbm] * 5,
        out_specs=(vm,) * 3,
        scratch_shapes=[
            V((3, CELLS + 2 * PAD2, CH), BF), V((3, CELLS + 2 * PAD1, CH), BF),
            V((2, LAT * W2, CH), BF), V((2, LAT * W2, CH), BF),
            V((2, LAT * W1, CH), BF), V((2, LAT * W1, CH), BF),
            V((CELLS, CH), BF), V((CELLS, CH), BF),
            V((ROWS, CH), BF), V((ROWS, CH), BF),
            V((3, 3 * CH, CH), BF), V((3, 3 * CH, CH), BF),
            V((CH, CELLS), BF), V((CH, CELLS), BF),
            V((CELLS, CH), F32),
            V((2, ROWS, CH), F32), V((2, ROWS, CH), BF),
            V((2, 8, BLOCK, CH), BF),
            V((2, 2, 4, TOP, CH), BF), V((2, 2, 2, 4, REST, HALF), BF),
            V((2, 3, 2, TOP, CH), BF), V((2, 3, 4, REST, HALF), BF),
            V((2, 2, 2, TOP, HALF), BF), V((2, 4, REST, HALF), BF),
            V((2, 3, TOP, HALF), BF), V((2, 3, REST, HALF), BF),
            V((BLOCK + 16, HALF), F32),
            V((2, DPS, 16, HALF), BF), V((2, DPS - 1, 16, HALF), BF),
            D((5,)), D((2, 2)), D((2, 2, 2)), D((2,)), D((2,)), D((2, 2)), D((2, 2)),
            D((2, 2)), D((2, 2)), D((2,)), D((2,)),
            pltpu.SemaphoreType.REGULAR, pltpu.SemaphoreType.REGULAR,
        ],
        compiler_params=pltpu.CompilerParams(
            collective_id=0, has_side_effects=True, vmem_limit_bytes=53760 * 1024),
    )(cotangent.reshape(CELLS, CH), pre_act.reshape(CELLS, CH), inputs.reshape(CELLS, CH),
      first_weight, second_weight)
    dx, g1, g2 = pl.pallas_call(
        write_out,
        name="write_out",
        out_shape=outs,
        in_specs=[vm] * 3,
        out_specs=(any_,) * 3,
        scratch_shapes=[D((3,))],
        compiler_params=pltpu.CompilerParams(vmem_limit_bytes=1024 * 1024),
    )(*got)
    return dx.reshape(inputs.shape), g1, g2


def solution(mesh):
    whole = P("dp", None, "lon", None)
    return jax.shard_map(
        local, mesh=mesh, in_specs=(whole, whole, whole, P(), P()),
        out_specs=(whole, P(("lon", "dp")), P(("lon", "dp"))), check_vma=False)
```

```python
import jax
import jax.numpy as jnp
from jax import lax
from jax.experimental import pallas as pl
from jax.experimental.pallas import tpu as pltpu
from jax.sharding import PartitionSpec as P

BF = jnp.bfloat16
F32 = jnp.float32
LAT = 32
COLS = 48
CH = 256
HALF = 128
CELLS = LAT * COLS
LONS = 16
DPS = 16
ROWS = 9 * CH
BLOCK = ROWS // LONS
UNIT = BLOCK // DPS
PAD2 = 96
TOP = 64
REST = BLOCK - TOP
PAD1 = 64
W2 = 18
W1 = 12
M2 = 384
M1 = 256
MESH = pl.DeviceIdType.MESH
FAR_FIRST = sorted(range(1, DPS), key=lambda d: -min(d, DPS - d))
scope = jax.named_scope


def mm(a, b):
    return jnp.dot(a, b, preferred_element_type=F32)


def kernel(cot, pre2, x2, w1, w2, dx, g1, g2,
           V2, V1, S2, R2, S1, R1, pre, xin, w1b, w2b, wt1, wt2, hT, xT, acc,
           wf, wb, recvA, sY, sX, rY1, rX1, tY, tX, rY2, rX2, sC, sendD, recvD,
           ld, hs, hr, as_, ar, ys, yr, xs, xr, ds_, dr, know1, know2):
    lon = lax.axis_index("lon")
    dp = lax.axis_index("dp")
    core = lax.rem(lon, 2)
    y = lax.rem(lax.div(lon, 2), 4)
    xh = lax.div(lon, 8)
    left = lax.rem(lon + LONS - 1, LONS)
    right = lax.rem(lon + 1, LONS)
    partner = lon + 1 - 2 * core
    ypeer = [lax.rem(y + d, 4) for d in range(1, 4)]
    ylon = [xh * 8 + yp * 2 + core for yp in ypeer]
    xl = lax.rem(dp, 2)
    xat = [lax.rem(2 * xh + xl + e, 4) for e in range(1, 4)]
    xpeer = [(lax.div(a, 2), lax.rem(a, 2)) for a in xat]
    xid = [(h * 8 + y * 2 + core, dp - xl + l) for h, l in xpeer]
    dpeer = {d: lax.rem(dp + d, DPS) for d in range(1, DPS)}
    twin = dp + 1 - 2 * lax.rem(dp, 2)

    loads = []
    for i, (s, d) in enumerate((
        (cot, V2.at[1, PAD2:PAD2 + CELLS]), (w2, w2b), (pre2, pre), (x2, xin), (w1, w1b),
    )):
        c = pltpu.make_async_copy(s, d, ld.at[i])
        c.start()
        loads.append(c)

    barrier = pltpu.get_barrier_semaphore()

    def tell(sem, l, d):
        pl.semaphore_signal(sem, inc=1, device_id=(l, d), device_id_type=MESH)

    for l in [left, right] + ylon:
        tell(barrier, l, dp)
    for l, d in xid:
        tell(barrier, l, d)
    for d in (dpeer[2], dpeer[14], dpeer[4], dpeer[12]):
        tell(barrier, lon, d)

    for c in range(3):
        V2[c, 0:PAD2] = jnp.zeros((PAD2, CH), BF)
        V2[c, PAD2 + CELLS:] = jnp.zeros((PAD2, CH), BF)
        V1[c, 0:PAD1] = jnp.zeros((PAD1, CH), BF)
        V1[c, PAD1 + CELLS:] = jnp.zeros((PAD1, CH), BF)
    sC[BLOCK:] = jnp.zeros((16, HALF), F32)

    def remote(s, d, ss, rs, l, dd):
        c = pltpu.make_async_remote_copy(
            src_ref=s, dst_ref=d, send_sem=ss, recv_sem=rs,
            device_id=(l, dd), device_id_type=MESH)
        c.start()
        return c

    def wait_all(ref, sem):
        pltpu.make_async_copy(ref, ref, sem).wait()

    sent = []
    for g in range(2):
        sent.extend(((rX1.at[g], xs.at[g, 0]), (rY1.at[g], ys.at[g, 0])))
    at_wrap = (lon == 0) | (lon == 7) | (lon == 8) | (lon == 15)

    halves = (range(0, LAT // 2), range(LAT // 2, LAT))

    def pack(V, pad, S, w, lats=range(LAT)):
        for p in lats:
            o = pad + p * COLS
            S[0, p * w:(p + 1) * w] = V[1, o + COLS - w:o + COLS]
            S[1, p * w:(p + 1) * w] = V[1, o:o + w]

    def build_inner(V, pad, w):
        for p in range(LAT):
            o = pad + p * COLS
            V[0, o:o + COLS - w] = V[1, o + w:o + COLS]
            V[2, o + w:o + COLS] = V[1, o:o + COLS - w]

    early, late = 2 * core, 2 - 2 * core

    def build_edge(V, pad, R, w, i, first, q):
        n = LAT // 2 * w
        wait_all(R.at[1 - core if first else core, q * n:(q + 1) * n],
                 hr.at[i, 1 - core if first else core, q])

        @pl.when(core == (0 if first else 1))
        def _():
            for p in halves[q]:
                o = pad + p * COLS
                V[0, o + COLS - w:o + COLS] = R[1, p * w:(p + 1) * w]

        @pl.when(core == (1 if first else 0))
        def _():
            for p in halves[q]:
                o = pad + p * COLS
                V[2, o:o + w] = R[0, p * w:(p + 1) * w]

    def send_halo(S, R, i, q):
        n = S.shape[1] // 2
        rows = slice(q * n, (q + 1) * n)
        remote(S.at[0, rows], R.at[0, rows], hs.at[i, 0], hr.at[i, 0, q], right, dp)
        remote(S.at[1, rows], R.at[1, rows], hs.at[i, 1], hr.at[i, 1, q], left, dp)
        if q:
            sent.extend(((R.at[0], hs.at[i, 0]), (R.at[1], hs.at[i, 1])))

    with scope("ld0"):
        loads[0].wait()
    with scope("pack2"):
        pack(V2, PAD2, S2, W2)
    with scope("barrier"):
        pl.semaphore_wait(barrier, 12)
    for q in range(2):
        send_halo(S2, R2, 0, q)
    for d in (dpeer[4], dpeer[12]):
        tell(know1, lon, d)
    with scope("inner2"):
        build_inner(V2, PAD2, W2)

    def tr_weights(w, wt):
        for c in range(3):
            for r in range(3):
                k = 3 * r + c
                wt[c, r * CH:(r + 1) * CH] = w[k * CH:(k + 1) * CH].T

    with scope("trans2"):
        loads[1].wait()
        tr_weights(w2b, wt2)
        loads[2].wait()
        for i in range(6):
            rows = pl.ds(i * CH, CH)
            hT[:, rows] = jnp.maximum(pre[rows], jnp.zeros((CH, CH), BF)).T

    blocks2 = ((0, 768, ((0, 960), (1, 96))), (768, 768, ((1, 864), (2, 0))))
    blocks1 = ((0, 512, ((0, 640), (1, 64))),
               (512, 512, ((0, 1152), (1, 576), (2, 0))),
               (1024, 512, ((1, 1088), (2, 512))))

    def dx_part(V, wt, cols, block, i, m):
        taps = block[2]
        lhs, rhs = [], []
        for c in cols:
            for r, s in taps:
                lhs.append(V[c, pl.ds(pl.multiple_of(s + i * m, 16), m)])
            rhs.append(wt[c, taps[0][0] * CH:(taps[-1][0] + 1) * CH])
        return mm(jnp.concatenate(lhs, axis=1), jnp.concatenate(rhs, axis=0))

    def dx_loop(V, wt, cols, blocks, m, put):
        for b in blocks:
            @pl.loop(0, b[1] // m)
            def _(i, b=b):
                put(pl.multiple_of(b[0] + i * m, m), dx_part(V, wt, cols, b, i, m))

    cells2 = ((0, 768, 960), (0, 1536, 96), (768, 768, 0))
    cells1 = ((0, 1024, 640), (0, 1536, 64), (512, 1024, 0))

    def dw(g, srcT, V, cells, cols):
        for c in cols:
            for r in range(3):
                a, n, s = cells[r]
                v = mm(srcT[:, a:a + n], V[c, s:s + n])
                rows = pl.ds(pl.multiple_of((3 * r + c) * CH, CH), CH)
                wf[g, rows] = v
                wb[g, rows] = v.astype(BF)

    def dw_part(cells, last):
        for r in range(3):
            a, n, s = cells[r]
            v = mm(xT[:, a:a + n], V1[late, s:s + n])
            rows = pl.ds(pl.multiple_of((3 * r + late) * CH, CH), CH)
            if last:
                v = v + wf[0, rows]
                wb[0, rows] = v.astype(BF)
            wf[0, rows] = v

    def first2(m0, v):
        acc[pl.ds(m0, M2)] = v

    def more2(m0, v):
        acc[pl.ds(m0, M2)] += v

    def mask2(m0, v):
        rows = pl.ds(m0, M2)
        lg = jnp.where(pre[rows].astype(F32) > 0, acc[rows] + v, 0.0).astype(BF)
        V1[1, pl.ds(pl.multiple_of(PAD1 + m0, 16), M2)] = lg

    def first1(m0, v):
        acc[pl.ds(m0, M1)] = v

    def more1(m0, v):
        acc[pl.ds(m0, M1)] += v

    def only1(m0, v):
        dx[pl.ds(m0, M1)] = v.astype(BF)

    def last1(m0, v):
        rows = pl.ds(m0, M1)
        dx[rows] = (acc[rows] + v).astype(BF)

    with scope("dx2c"):
        dx_loop(V2, wt2, (1,), blocks2, M2, first2)
    with scope("dw2c"):
        dw(1, hT, V2, cells2, (1,))
    with scope("know1"):
        pl.semaphore_wait(know1, 2)
        tell(know2, lon, twin)
    with scope("trans1"):
        loads[3].wait()
        for i in range(6):
            rows = pl.ds(i * CH, CH)
            xT[:, rows] = xin[rows].T
        loads[4].wait()
        tr_weights(w1b, wt1)

    with scope("halo2e"):
        for q in range(2):
            build_edge(V2, PAD2, R2, W2, 0, True, q)
    with scope("dx2e"):
        dx_loop(V2, wt2, (early,), blocks2, M2, more2)
    with scope("dw2e"):
        dw(1, hT, V2, cells2, (early,))
    with scope("halo2l"):
        build_edge(V2, PAD2, R2, W2, 0, False, 0)
    with scope("dx2l"):
        dx_loop(V2, wt2, (late,), ((0, 768, ((1, 96),)), (768, 768, ((2, 0),))), M2, more2)
    with scope("halo2m"):
        build_edge(V2, PAD2, R2, W2, 0, False, 1)
    for q, b in enumerate(((0, 768, ((0, 960),)), (768, 768, ((1, 864),)))):
        with scope("dx2m%d" % q):
            dx_loop(V2, wt2, (late,), (b,), M2, mask2)
        with scope("pack1%d" % q):
            pack(V1, PAD1, S1, W1, halves[q])
        send_halo(S1, R1, 1, q)
    with scope("dw2l"):
        dw(1, hT, V2, cells2, (late,))

    def stage_a(g):
        for j in range(8):
            rows = pl.ds(pl.multiple_of((2 * j + 1 - core) * BLOCK, 16), BLOCK)
            remote(wb.at[g, rows], recvA.at[g, j], as_.at[g], ar.at[g], partner, dp)
        sent.append((recvA.at[g], as_.at[g]))

    def send_taps(ready):
        for v in range(2):
            @pl.when(core == v)
            def _(v=v):
                for c in (1, 2 * v) if ready else (2 - 2 * v,):
                    for k in (c, 3 + c, 6 + c):
                        for b in range(1 - v, LONS, 2):
                            lo, hi = max(k * CH, b * BLOCK), min((k + 1) * CH, (b + 1) * BLOCK)
                            if lo < hi:
                                remote(wb.at[0, lo:hi], recvA.at[0, b // 2, lo - b * BLOCK:hi - b * BLOCK],
                                       as_.at[0], ar.at[0], partner, dp)

    def stage_b(g):
        wait_all(recvA.at[g], ar.at[g])

        @pl.loop(0, 8)
        def _(j):
            rows = pl.ds(pl.multiple_of((2 * j + core) * BLOCK, 16), BLOCK)
            v = (wf[g, rows] + recvA[g, j].astype(F32)).astype(BF)
            h, yy = lax.div(j, 4), lax.rem(j, 4)
            sY[g, h, yy] = v[:TOP]
            sX[g, h, 0, yy] = v[TOP:, :HALF]
            sX[g, h, 1, yy] = v[TOP:, HALF:]

        for e in (1, 0, 2):
            h, l = xpeer[e]
            remote(sX.at[g, h, l], rX1.at[g, e], xs.at[g, 0], xr.at[g, 0], *xid[e])
        for d in (1, 0, 2):
            remote(sY.at[g, :, ypeer[d]], rY1.at[g, d], ys.at[g, 0], yr.at[g, 0], ylon[d], dp)
    def stage_cy(g):
        wait_all(rY1.at[g], yr.at[g, 0])
        for h in range(2):
            v = sY[g, h, y].astype(F32)
            for d in range(3):
                v = v + rY1[g, d, h].astype(F32)
            v = v.astype(BF)
            tY[g, h, 0] = v[:, :HALF]
            tY[g, h, 1] = v[:, HALF:]
        for e in (1, 0, 2):
            h, l = xpeer[e]
            remote(tY.at[g, h, l], rY2.at[g, e], xs.at[g, 1], xr.at[g, 1], *xid[e])
        sent.append((rY2.at[g], xs.at[g, 1]))

    def stage_cx(g):
        wait_all(rX1.at[g], xr.at[g, 0])
        for i in range(4):
            v = sX[g, xh, xl, i].astype(F32)
            for e in range(3):
                v = v + rX1[g, e, i].astype(F32)
            tX[g, i] = v.astype(BF)
        for d in (1, 0, 2):
            remote(tX.at[g, ypeer[d]], rX2.at[g, d], ys.at[g, 1], yr.at[g, 1], ylon[d], dp)
        sent.append((rX2.at[g], ys.at[g, 1]))

    def stage_d(g):
        wait_all(rY2.at[g], xr.at[g, 1])
        v = tY[g, xh, xl].astype(F32)
        for e in range(3):
            v = v + rY2[g, e].astype(F32)
        sC[0:TOP] = v
        wait_all(rX2.at[g], yr.at[g, 1])
        v = tX[g, y].astype(F32)
        for d in range(3):
            v = v + rX2[g, d].astype(F32)
        sC[TOP:BLOCK] = v
        for u in range(DPS):
            sendD[g, u] = sC[u * UNIT:u * UNIT + 16].astype(BF)
        for d in FAR_FIRST:
            remote(sendD.at[g, dpeer[d]], recvD.at[g, d - 1], ds_.at[g], dr.at[g], lon, dpeer[d])
        sent.append((recvD.at[g], ds_.at[g]))

    norm = float(16 * LAT * 768) ** -0.5

    def finish(g, out):
        wait_all(recvD.at[g], dr.at[g])
        mine = sendD[g, dp].astype(F32)
        for d in range(2, DPS, 2):
            mine = mine + recvD[g, d - 1].astype(F32)
        other = recvD[g, 0].astype(F32)
        for d in range(3, DPS, 2):
            other = other + recvD[g, d - 1].astype(F32)
        for h, v in enumerate((jnp.where(xl == 0, mine, other), jnp.where(xl == 0, other, mine))):
            v = v * norm
            for u in range(UNIT):
                out[pl.ds(u * CH + h * HALF, HALF)] = v[u]

    stage_a(1)
    with scope("inner1"):
        build_inner(V1, PAD1, W1)
    with scope("dw1c"):
        dw(0, xT, V1, cells1, (1,))
    with scope("halo1e"):
        for q in range(2):
            build_edge(V1, PAD1, R1, W1, 1, True, q)
    with scope("dw1e"):
        dw(0, xT, V1, cells1, (early,))
    send_taps(True)
    @pl.when(at_wrap)
    def _():
        stage_b(1)

    with scope("halo1l"):
        build_edge(V1, PAD1, R1, W1, 1, False, 0)
    with scope("dw1l"):
        dw_part(((0, 128, 640), (0, 768, 64), (512, 768, 0)), False)
    with scope("halo1m"):
        build_edge(V1, PAD1, R1, W1, 1, False, 1)
    with scope("dw1m"):
        dw_part(((128, 896, 768), (768, 768, 832), (1280, 256, 768)), True)
    send_taps(False)
    sent.append((recvA.at[0], as_.at[0]))
    @pl.when(jnp.logical_not(at_wrap))
    def _():
        stage_b(1)

    with scope("dx1a"):
        dx_loop(V1, wt1, (0, 1, 2), blocks1[:1], M1, only1)
    with scope("b1"):
        stage_b(0)
    with scope("dx1b"):
        dx_loop(V1, wt1, (0, 1, 2), blocks1[1:], M1, only1)
    with scope("c2y"):
        stage_cy(1)
    with scope("c2x"):
        stage_cx(1)
    with scope("c1y"):
        stage_cy(0)
    with scope("c1x"):
        stage_cx(0)
    with scope("know2"):
        pl.semaphore_wait(know2, 1)
    with scope("d2"):
        stage_d(1)
    with scope("d1"):
        stage_d(0)
    with scope("f2"):
        finish(1, g2)
    with scope("f1"):
        finish(0, g1)
    with scope("sends"):
        for ref, sem in sent:
            wait_all(ref, sem)


def write_out(dx, g1, g2, dxo, g1o, g2o, sem):
    copies = [pltpu.make_async_copy(s, d, sem.at[i])
              for i, (s, d) in enumerate(((g1, g1o), (g2, g2o), (dx, dxo)))]
    for c in copies:
        c.start()
    for c in copies:
        c.wait()


def local(inputs, pre_act, cotangent, first_weight, second_weight):
    hbm = pl.BlockSpec(memory_space=pltpu.HBM)
    vm = pl.BlockSpec(memory_space=pltpu.VMEM)
    any_ = pl.BlockSpec(memory_space=pl.ANY)
    V = pltpu.VMEM
    D = pltpu.SemaphoreType.DMA
    outs = (
        jax.ShapeDtypeStruct((CELLS, CH), BF),
        jax.ShapeDtypeStruct((UNIT * CH,), F32),
        jax.ShapeDtypeStruct((UNIT * CH,), F32),
    )
    got = pl.pallas_call(
        kernel,
        name="conv_back",
        out_shape=outs,
        in_specs=[hbm] * 5,
        out_specs=(vm,) * 3,
        scratch_shapes=[
            V((3, CELLS + 2 * PAD2, CH), BF), V((3, CELLS + 2 * PAD1, CH), BF),
            V((2, LAT * W2, CH), BF), V((2, LAT * W2, CH), BF),
            V((2, LAT * W1, CH), BF), V((2, LAT * W1, CH), BF),
            V((CELLS, CH), BF), V((CELLS, CH), BF),
            V((ROWS, CH), BF), V((ROWS, CH), BF),
            V((3, 3 * CH, CH), BF), V((3, 3 * CH, CH), BF),
            V((CH, CELLS), BF), V((CH, CELLS), BF),
            V((CELLS, CH), F32),
            V((2, ROWS, CH), F32), V((2, ROWS, CH), BF),
            V((2, 8, BLOCK, CH), BF),
            V((2, 2, 4, TOP, CH), BF), V((2, 2, 2, 4, REST, HALF), BF),
            V((2, 3, 2, TOP, CH), BF), V((2, 3, 4, REST, HALF), BF),
            V((2, 2, 2, TOP, HALF), BF), V((2, 4, REST, HALF), BF),
            V((2, 3, TOP, HALF), BF), V((2, 3, REST, HALF), BF),
            V((BLOCK + 16, HALF), F32),
            V((2, DPS, 16, HALF), BF), V((2, DPS - 1, 16, HALF), BF),
            D((5,)), D((2, 2)), D((2, 2, 2)), D((2,)), D((2,)), D((2, 2)), D((2, 2)),
            D((2, 2)), D((2, 2)), D((2,)), D((2,)),
            pltpu.SemaphoreType.REGULAR, pltpu.SemaphoreType.REGULAR,
        ],
        compiler_params=pltpu.CompilerParams(
            collective_id=0, has_side_effects=True, vmem_limit_bytes=53760 * 1024),
    )(cotangent.reshape(CELLS, CH), pre_act.reshape(CELLS, CH), inputs.reshape(CELLS, CH),
      first_weight, second_weight)
    dx, g1, g2 = pl.pallas_call(
        write_out,
        name="write_out",
        out_shape=outs,
        in_specs=[vm] * 3,
        out_specs=(any_,) * 3,
        scratch_shapes=[D((3,))],
        compiler_params=pltpu.CompilerParams(vmem_limit_bytes=1024 * 1024),
    )(*got)
    return dx.reshape(inputs.shape), g1, g2


def solution(mesh):
    whole = P("dp", None, "lon", None)
    return jax.shard_map(
        local, mesh=mesh, in_specs=(whole, whole, whole, P(), P()),
        out_specs=(whole, P(("lon", "dp")), P(("lon", "dp"))), check_vma=False)
```

```python
import jax
import jax.numpy as jnp
from jax import lax
from jax.experimental import pallas as pl
from jax.experimental.pallas import tpu as pltpu
from jax.sharding import PartitionSpec as P

BF = jnp.bfloat16
F32 = jnp.float32
LAT = 32
COLS = 48
CH = 256
HALF = 128
CELLS = LAT * COLS
LONS = 16
DPS = 16
ROWS = 9 * CH
BLOCK = ROWS // LONS
UNIT = BLOCK // DPS
PAD2 = 96
TOP = 64
REST = BLOCK - TOP
PAD1 = 64
W2 = 18
W1 = 12
M2 = 384
M1 = 256
MESH = pl.DeviceIdType.MESH
FAR_FIRST = sorted(range(1, DPS), key=lambda d: -min(d, DPS - d))
scope = jax.named_scope


def mm(a, b):
    return jnp.dot(a, b, preferred_element_type=F32)


def kernel(cot, pre2, x2, w1, w2, dx, g1, g2,
           V2, V1, S2, R2, S1, R1, pre, xin, w1b, w2b, wt1, wt2, hT, xT, acc,
           wf, wb, recvA, sY, sX, rY1, rX1, tY, tX, rY2, rX2, sC, sendD, recvD,
           ld, hs, hr, as_, ar, ys, yr, xs, xr, ds_, dr, know1, know2):
    lon = lax.axis_index("lon")
    dp = lax.axis_index("dp")
    core = lax.rem(lon, 2)
    y = lax.rem(lax.div(lon, 2), 4)
    xh = lax.div(lon, 8)
    left = lax.rem(lon + LONS - 1, LONS)
    right = lax.rem(lon + 1, LONS)
    partner = lon + 1 - 2 * core
    ypeer = [lax.rem(y + d, 4) for d in range(1, 4)]
    ylon = [xh * 8 + yp * 2 + core for yp in ypeer]
    xl = lax.rem(dp, 2)
    xat = [lax.rem(2 * xh + xl + e, 4) for e in range(1, 4)]
    xpeer = [(lax.div(a, 2), lax.rem(a, 2)) for a in xat]
    xid = [(h * 8 + y * 2 + core, dp - xl + l) for h, l in xpeer]
    dpeer = {d: lax.rem(dp + d, DPS) for d in range(1, DPS)}
    twin = dp + 1 - 2 * lax.rem(dp, 2)

    loads = []
    for i, (s, d) in enumerate((
        (cot, V2.at[1, PAD2:PAD2 + CELLS]), (w2, w2b), (pre2, pre), (x2, xin), (w1, w1b),
    )):
        c = pltpu.make_async_copy(s, d, ld.at[i])
        c.start()
        loads.append(c)

    barrier = pltpu.get_barrier_semaphore()

    def tell(sem, l, d):
        pl.semaphore_signal(sem, inc=1, device_id=(l, d), device_id_type=MESH)

    for l in [left, right] + ylon:
        tell(barrier, l, dp)
    for l, d in xid:
        tell(barrier, l, d)
    for d in (dpeer[2], dpeer[14], dpeer[4], dpeer[12]):
        tell(barrier, lon, d)

    for c in range(3):
        V2[c, 0:PAD2] = jnp.zeros((PAD2, CH), BF)
        V2[c, PAD2 + CELLS:] = jnp.zeros((PAD2, CH), BF)
        V1[c, 0:PAD1] = jnp.zeros((PAD1, CH), BF)
        V1[c, PAD1 + CELLS:] = jnp.zeros((PAD1, CH), BF)
    sC[BLOCK:] = jnp.zeros((16, HALF), F32)

    def remote(s, d, ss, rs, l, dd):
        c = pltpu.make_async_remote_copy(
            src_ref=s, dst_ref=d, send_sem=ss, recv_sem=rs,
            device_id=(l, dd), device_id_type=MESH)
        c.start()
        return c

    def wait_all(ref, sem):
        pltpu.make_async_copy(ref, ref, sem).wait()

    sent = []
    for g in range(2):
        sent.extend(((rX1.at[g], xs.at[g, 0]), (rY1.at[g], ys.at[g, 0])))
    at_wrap = (lon == 0) | (lon == 7) | (lon == 8) | (lon == 15)

    halves = (range(0, LAT // 2), range(LAT // 2, LAT))

    def pack(V, pad, S, w, lats=range(LAT)):
        for p in lats:
            o = pad + p * COLS
            S[0, p * w:(p + 1) * w] = V[1, o + COLS - w:o + COLS]
            S[1, p * w:(p + 1) * w] = V[1, o:o + w]

    def build_inner(V, pad, w):
        for p in range(LAT):
            o = pad + p * COLS
            V[0, o:o + COLS - w] = V[1, o + w:o + COLS]
            V[2, o + w:o + COLS] = V[1, o:o + COLS - w]

    early, late = 2 * core, 2 - 2 * core

    def build_edge(V, pad, R, w, i, first, q):
        n = LAT // 2 * w
        wait_all(R.at[1 - core if first else core, q * n:(q + 1) * n],
                 hr.at[i, 1 - core if first else core, q])

        @pl.when(core == (0 if first else 1))
        def _():
            for p in halves[q]:
                o = pad + p * COLS
                V[0, o + COLS - w:o + COLS] = R[1, p * w:(p + 1) * w]

        @pl.when(core == (1 if first else 0))
        def _():
            for p in halves[q]:
                o = pad + p * COLS
                V[2, o:o + w] = R[0, p * w:(p + 1) * w]

    def send_halo(S, R, i, q):
        n = S.shape[1] // 2
        rows = slice(q * n, (q + 1) * n)
        remote(S.at[0, rows], R.at[0, rows], hs.at[i, 0], hr.at[i, 0, q], right, dp)
        remote(S.at[1, rows], R.at[1, rows], hs.at[i, 1], hr.at[i, 1, q], left, dp)
        if q:
            sent.extend(((R.at[0], hs.at[i, 0]), (R.at[1], hs.at[i, 1])))

    with scope("ld0"):
        loads[0].wait()
    with scope("pack2"):
        pack(V2, PAD2, S2, W2)
    with scope("barrier"):
        pl.semaphore_wait(barrier, 12)
    for q in range(2):
        send_halo(S2, R2, 0, q)
    for d in (dpeer[4], dpeer[12]):
        tell(know1, lon, d)
    with scope("inner2"):
        build_inner(V2, PAD2, W2)

    def tr_weights(w, wt):
        for c in range(3):
            for r in range(3):
                k = 3 * r + c
                wt[c, r * CH:(r + 1) * CH] = w[k * CH:(k + 1) * CH].T

    with scope("trans2"):
        loads[1].wait()
        tr_weights(w2b, wt2)
        loads[2].wait()
        for i in range(6):
            rows = pl.ds(i * CH, CH)
            hT[:, rows] = jnp.maximum(pre[rows], jnp.zeros((CH, CH), BF)).T

    blocks2 = ((0, 768, ((0, 960), (1, 96))), (768, 768, ((1, 864), (2, 0))))
    blocks1 = ((0, 512, ((0, 640), (1, 64))),
               (512, 512, ((0, 1152), (1, 576), (2, 0))),
               (1024, 512, ((1, 1088), (2, 512))))

    def dx_part(V, wt, cols, block, i, m):
        taps = block[2]
        lhs, rhs = [], []
        for c in cols:
            for r, s in taps:
                lhs.append(V[c, pl.ds(pl.multiple_of(s + i * m, 16), m)])
            rhs.append(wt[c, taps[0][0] * CH:(taps[-1][0] + 1) * CH])
        return mm(jnp.concatenate(lhs, axis=1), jnp.concatenate(rhs, axis=0))

    def dx_loop(V, wt, cols, blocks, m, put):
        for b in blocks:
            @pl.loop(0, b[1] // m)
            def _(i, b=b):
                put(pl.multiple_of(b[0] + i * m, m), dx_part(V, wt, cols, b, i, m))

    cells2 = ((0, 768, 960), (0, 1536, 96), (768, 768, 0))
    cells1 = ((0, 1024, 640), (0, 1536, 64), (512, 1024, 0))

    def dw(g, srcT, V, cells, cols):
        for c in cols:
            for r in range(3):
                a, n, s = cells[r]
                v = mm(srcT[:, a:a + n], V[c, s:s + n])
                rows = pl.ds(pl.multiple_of((3 * r + c) * CH, CH), CH)
                wf[g, rows] = v
                wb[g, rows] = v.astype(BF)

    def dw_part(cells, last):
        for r in range(3):
            a, n, s = cells[r]
            v = mm(xT[:, a:a + n], V1[late, s:s + n])
            rows = pl.ds(pl.multiple_of((3 * r + late) * CH, CH), CH)
            if last:
                v = v + wf[0, rows]
                wb[0, rows] = v.astype(BF)
            wf[0, rows] = v

    def first2(m0, v):
        acc[pl.ds(m0, M2)] = v

    def more2(m0, v):
        acc[pl.ds(m0, M2)] += v

    def mask2(m0, v):
        rows = pl.ds(m0, M2)
        lg = jnp.where(pre[rows].astype(F32) > 0, acc[rows] + v, 0.0).astype(BF)
        V1[1, pl.ds(pl.multiple_of(PAD1 + m0, 16), M2)] = lg

    def first1(m0, v):
        acc[pl.ds(m0, M1)] = v

    def more1(m0, v):
        acc[pl.ds(m0, M1)] += v

    def only1(m0, v):
        dx[pl.ds(m0, M1)] = v.astype(BF)

    def last1(m0, v):
        rows = pl.ds(m0, M1)
        dx[rows] = (acc[rows] + v).astype(BF)

    with scope("dx2c"):
        dx_loop(V2, wt2, (1,), blocks2, M2, first2)
    with scope("dw2c"):
        dw(1, hT, V2, cells2, (1,))
    with scope("know1"):
        pl.semaphore_wait(know1, 2)
        tell(know2, lon, twin)
    with scope("trans1"):
        loads[3].wait()
        for i in range(6):
            rows = pl.ds(i * CH, CH)
            xT[:, rows] = xin[rows].T
        loads[4].wait()
        tr_weights(w1b, wt1)

    with scope("halo2e"):
        for q in range(2):
            build_edge(V2, PAD2, R2, W2, 0, True, q)
    with scope("dx2e"):
        dx_loop(V2, wt2, (early,), blocks2, M2, more2)
    with scope("dw2e"):
        dw(1, hT, V2, cells2, (early,))
    with scope("halo2l"):
        build_edge(V2, PAD2, R2, W2, 0, False, 0)
    with scope("dx2l"):
        dx_loop(V2, wt2, (late,), ((0, 768, ((1, 96),)), (768, 768, ((2, 0),))), M2, more2)
    with scope("halo2m"):
        build_edge(V2, PAD2, R2, W2, 0, False, 1)
    for q, b in enumerate(((0, 768, ((0, 960),)), (768, 768, ((1, 864),)))):
        with scope("dx2m%d" % q):
            dx_loop(V2, wt2, (late,), (b,), M2, mask2)
        with scope("pack1%d" % q):
            pack(V1, PAD1, S1, W1, halves[q])
        send_halo(S1, R1, 1, q)
    with scope("dw2l"):
        dw(1, hT, V2, cells2, (late,))

    def stage_a(g):
        for j in range(8):
            rows = pl.ds(pl.multiple_of((2 * j + 1 - core) * BLOCK, 16), BLOCK)
            remote(wb.at[g, rows], recvA.at[g, j], as_.at[g], ar.at[g], partner, dp)
        sent.append((recvA.at[g], as_.at[g]))

    def send_taps(ready):
        for v in range(2):
            @pl.when(core == v)
            def _(v=v):
                for c in (1, 2 * v) if ready else (2 - 2 * v,):
                    for k in (c, 3 + c, 6 + c):
                        for b in range(1 - v, LONS, 2):
                            lo, hi = max(k * CH, b * BLOCK), min((k + 1) * CH, (b + 1) * BLOCK)
                            if lo < hi:
                                remote(wb.at[0, lo:hi], recvA.at[0, b // 2, lo - b * BLOCK:hi - b * BLOCK],
                                       as_.at[0], ar.at[0], partner, dp)

    def stage_b(g):
        wait_all(recvA.at[g], ar.at[g])

        @pl.loop(0, 8)
        def _(j):
            rows = pl.ds(pl.multiple_of((2 * j + core) * BLOCK, 16), BLOCK)
            v = (wf[g, rows] + recvA[g, j].astype(F32)).astype(BF)
            h, yy = lax.div(j, 4), lax.rem(j, 4)
            sY[g, h, yy] = v[:TOP]
            sX[g, h, 0, yy] = v[TOP:, :HALF]
            sX[g, h, 1, yy] = v[TOP:, HALF:]

        for e in (1, 0, 2):
            h, l = xpeer[e]
            remote(sX.at[g, h, l], rX1.at[g, e], xs.at[g, 0], xr.at[g, 0], *xid[e])
        for d in (1, 0, 2):
            remote(sY.at[g, :, ypeer[d]], rY1.at[g, d], ys.at[g, 0], yr.at[g, 0], ylon[d], dp)
    def stage_cy(g):
        wait_all(rY1.at[g], yr.at[g, 0])
        for h in range(2):
            v = sY[g, h, y].astype(F32)
            for d in range(3):
                v = v + rY1[g, d, h].astype(F32)
            v = v.astype(BF)
            tY[g, h, 0] = v[:, :HALF]
            tY[g, h, 1] = v[:, HALF:]
        for e in (1, 0, 2):
            h, l = xpeer[e]
            remote(tY.at[g, h, l], rY2.at[g, e], xs.at[g, 1], xr.at[g, 1], *xid[e])
        sent.append((rY2.at[g], xs.at[g, 1]))

    def stage_cx(g):
        wait_all(rX1.at[g], xr.at[g, 0])
        for i in range(4):
            v = sX[g, xh, xl, i].astype(F32)
            for e in range(3):
                v = v + rX1[g, e, i].astype(F32)
            tX[g, i] = v.astype(BF)
        for d in (1, 0, 2):
            remote(tX.at[g, ypeer[d]], rX2.at[g, d], ys.at[g, 1], yr.at[g, 1], ylon[d], dp)
        sent.append((rX2.at[g], ys.at[g, 1]))

    def stage_d(g):
        wait_all(rY2.at[g], xr.at[g, 1])
        v = tY[g, xh, xl].astype(F32)
        for e in range(3):
            v = v + rY2[g, e].astype(F32)
        sC[0:TOP] = v
        wait_all(rX2.at[g], yr.at[g, 1])
        v = tX[g, y].astype(F32)
        for d in range(3):
            v = v + rX2[g, d].astype(F32)
        sC[TOP:BLOCK] = v
        for u in range(DPS):
            sendD[g, u] = sC[u * UNIT:u * UNIT + 16].astype(BF)
        for d in FAR_FIRST:
            remote(sendD.at[g, dpeer[d]], recvD.at[g, d - 1], ds_.at[g], dr.at[g], lon, dpeer[d])
        sent.append((recvD.at[g], ds_.at[g]))

    norm = float(16 * LAT * 768) ** -0.5

    def finish(g, out):
        wait_all(recvD.at[g], dr.at[g])
        mine = sendD[g, dp].astype(F32)
        for d in range(2, DPS, 2):
            mine = mine + recvD[g, d - 1].astype(F32)
        other = recvD[g, 0].astype(F32)
        for d in range(3, DPS, 2):
            other = other + recvD[g, d - 1].astype(F32)
        for h, v in enumerate((jnp.where(xl == 0, mine, other), jnp.where(xl == 0, other, mine))):
            v = v * norm
            for u in range(UNIT):
                out[pl.ds(u * CH + h * HALF, HALF)] = v[u]

    stage_a(1)
    with scope("inner1"):
        build_inner(V1, PAD1, W1)
    with scope("dw1c"):
        dw(0, xT, V1, cells1, (1,))
    with scope("halo1e"):
        for q in range(2):
            build_edge(V1, PAD1, R1, W1, 1, True, q)
    with scope("dw1e"):
        dw(0, xT, V1, cells1, (early,))
    send_taps(True)
    @pl.when(at_wrap)
    def _():
        stage_b(1)

    with scope("halo1l"):
        build_edge(V1, PAD1, R1, W1, 1, False, 0)
    with scope("dw1l"):
        dw_part(((0, 128, 640), (0, 768, 64), (512, 768, 0)), False)
    with scope("halo1m"):
        build_edge(V1, PAD1, R1, W1, 1, False, 1)
    with scope("dw1m"):
        dw_part(((128, 896, 768), (768, 768, 832), (1280, 256, 768)), True)
    send_taps(False)
    sent.append((recvA.at[0], as_.at[0]))
    @pl.when(jnp.logical_not(at_wrap))
    def _():
        stage_b(1)

    with scope("b1"):
        stage_b(0)
    with scope("dx1b"):
        dx_loop(V1, wt1, (0, 1, 2), blocks1[:], M1, only1)
    with scope("c2y"):
        stage_cy(1)
    with scope("c2x"):
        stage_cx(1)
    with scope("c1y"):
        stage_cy(0)
    with scope("c1x"):
        stage_cx(0)
    with scope("know2"):
        pl.semaphore_wait(know2, 1)
    with scope("d2"):
        stage_d(1)
    with scope("d1"):
        stage_d(0)
    with scope("f2"):
        finish(1, g2)
    with scope("f1"):
        finish(0, g1)
    with scope("sends"):
        for ref, sem in sent:
            wait_all(ref, sem)


def write_out(dx, g1, g2, dxo, g1o, g2o, sem):
    copies = [pltpu.make_async_copy(s, d, sem.at[i])
              for i, (s, d) in enumerate(((g1, g1o), (g2, g2o), (dx, dxo)))]
    for c in copies:
        c.start()
    for c in copies:
        c.wait()


def local(inputs, pre_act, cotangent, first_weight, second_weight):
    hbm = pl.BlockSpec(memory_space=pltpu.HBM)
    vm = pl.BlockSpec(memory_space=pltpu.VMEM)
    any_ = pl.BlockSpec(memory_space=pl.ANY)
    V = pltpu.VMEM
    D = pltpu.SemaphoreType.DMA
    outs = (
        jax.ShapeDtypeStruct((CELLS, CH), BF),
        jax.ShapeDtypeStruct((UNIT * CH,), F32),
        jax.ShapeDtypeStruct((UNIT * CH,), F32),
    )
    got = pl.pallas_call(
        kernel,
        name="conv_back",
        out_shape=outs,
        in_specs=[hbm] * 5,
        out_specs=(vm,) * 3,
        scratch_shapes=[
            V((3, CELLS + 2 * PAD2, CH), BF), V((3, CELLS + 2 * PAD1, CH), BF),
            V((2, LAT * W2, CH), BF), V((2, LAT * W2, CH), BF),
            V((2, LAT * W1, CH), BF), V((2, LAT * W1, CH), BF),
            V((CELLS, CH), BF), V((CELLS, CH), BF),
            V((ROWS, CH), BF), V((ROWS, CH), BF),
            V((3, 3 * CH, CH), BF), V((3, 3 * CH, CH), BF),
            V((CH, CELLS), BF), V((CH, CELLS), BF),
            V((CELLS, CH), F32),
            V((2, ROWS, CH), F32), V((2, ROWS, CH), BF),
            V((2, 8, BLOCK, CH), BF),
            V((2, 2, 4, TOP, CH), BF), V((2, 2, 2, 4, REST, HALF), BF),
            V((2, 3, 2, TOP, CH), BF), V((2, 3, 4, REST, HALF), BF),
            V((2, 2, 2, TOP, HALF), BF), V((2, 4, REST, HALF), BF),
            V((2, 3, TOP, HALF), BF), V((2, 3, REST, HALF), BF),
            V((BLOCK + 16, HALF), F32),
            V((2, DPS, 16, HALF), BF), V((2, DPS - 1, 16, HALF), BF),
            D((5,)), D((2, 2)), D((2, 2, 2)), D((2,)), D((2,)), D((2, 2)), D((2, 2)),
            D((2, 2)), D((2, 2)), D((2,)), D((2,)),
            pltpu.SemaphoreType.REGULAR, pltpu.SemaphoreType.REGULAR,
        ],
        compiler_params=pltpu.CompilerParams(
            collective_id=0, has_side_effects=True, vmem_limit_bytes=53760 * 1024),
    )(cotangent.reshape(CELLS, CH), pre_act.reshape(CELLS, CH), inputs.reshape(CELLS, CH),
      first_weight, second_weight)
    dx, g1, g2 = pl.pallas_call(
        write_out,
        name="write_out",
        out_shape=outs,
        in_specs=[vm] * 3,
        out_specs=(any_,) * 3,
        scratch_shapes=[D((3,))],
        compiler_params=pltpu.CompilerParams(vmem_limit_bytes=1024 * 1024),
    )(*got)
    return dx.reshape(inputs.shape), g1, g2


def solution(mesh):
    whole = P("dp", None, "lon", None)
    return jax.shard_map(
        local, mesh=mesh, in_specs=(whole, whole, whole, P(), P()),
        out_specs=(whole, P(("lon", "dp")), P(("lon", "dp"))), check_vma=False)
```
